128 devices in a mesh: rep: 1, fsdp: 2 (over core), ep: 64 (over z, y, x).
Axes of the slice: x: 4, y: 4, z: 4, core: 2. Of those that a mesh axis runs over, the one named last changes fastest.
Arguments:
- tokens: bfloat16 [32768, 2048], P(('rep', 'ep', 'fsdp'))
- expert_idx: int32 [32768, 6], P(('rep', 'ep', 'fsdp'))
- gates: float32 [32768, 6], P(('rep', 'ep', 'fsdp'))
- w_gate: bfloat16 [64, 2048, 1408], P('ep', 'fsdp')
- w_up: bfloat16 [64, 2048, 1408], P('ep', 'fsdp')
- w_down: bfloat16 [64, 1408, 2048], P('ep', None, 'fsdp')
Outputs:
- output: bfloat16 [32768, 2048], P(('rep', 'ep', 'fsdp'))
All inputs are finite; a program needn't handle non-finite values.
Results may differ from the reference program's by a relative error of at most 0.00138.
Values are sent between devices in bfloat16 or wider.
A program may use at most 1 GiB of HBM per device.

```python
import jax
import jax.numpy as jnp
from jax import lax

TOK_DEV = 256
MODEL_DIM = 2048
FFN_DIM = 1408
NUM_EXPERTS = 64
TOP_K = 6
EP_SIZE = 64
FSDP_SIZE = 2

GROUP_DEVS = EP_SIZE * FSDP_SIZE
ROW_COUNT = GROUP_DEVS * TOK_DEV
CAPACITY = (2 * TOK_DEV * TOP_K + NUM_EXPERTS - 1) // NUM_EXPERTS


def route_draw(key):
    key_rank, key_noise = jax.random.split(key)
    ranks = jax.random.permutation(key_rank, NUM_EXPERTS)
    skew = (ranks * 768) // NUM_EXPERTS
    noise = jax.random.randint(key_noise, (ROW_COUNT, NUM_EXPERTS), 0, 1024)
    scores = (noise + skew[None, :]) * NUM_EXPERTS + jnp.arange(NUM_EXPERTS)[None, :]
    top_vals, chosen = lax.top_k(scores, TOP_K)
    return chosen.astype(jnp.int32)


def setup_inputs(seed: int = 0, part: int = 0) -> dict:
    part_key = jax.random.fold_in(jax.random.key(seed), part)
    key_tok, key_route, key_gate = jax.random.split(part_key, 3)
    key_wg, key_wu, key_wd = jax.random.split(jax.random.key(seed + 1), 3)
    tokens = jax.random.normal(key_tok, (ROW_COUNT, MODEL_DIM), jnp.float32).astype(jnp.bfloat16)
    expert_idx = route_draw(key_route)
    gates = jax.random.uniform(key_gate, (ROW_COUNT, TOP_K), jnp.float32, 0.2, 0.8)
    w_gate = (jax.random.normal(key_wg, (NUM_EXPERTS, MODEL_DIM, FFN_DIM), jnp.float32) * MODEL_DIM ** -0.5).astype(jnp.bfloat16)
    w_up = (jax.random.normal(key_wu, (NUM_EXPERTS, MODEL_DIM, FFN_DIM), jnp.float32) * MODEL_DIM ** -0.5).astype(jnp.bfloat16)
    w_down = (jax.random.normal(key_wd, (NUM_EXPERTS, FFN_DIM, MODEL_DIM), jnp.float32) * (2.0 * FFN_DIM ** -0.5)).astype(jnp.bfloat16)
    return {'tokens': tokens, 'expert_idx': expert_idx, 'gates': gates, 'w_gate': w_gate, 'w_up': w_up, 'w_down': w_down}


def block_slots(idx_block):
    flat_ids = idx_block.reshape(TOK_DEV * TOP_K)
    onehot = (flat_ids[:, None] == jnp.arange(NUM_EXPERTS)[None, :]).astype(jnp.int32)
    before = jnp.cumsum(onehot, axis=0) - onehot
    return jnp.sum(before * onehot, axis=1)


def reference(tokens, expert_idx, gates, w_gate, w_up, w_down):
    pair_count = ROW_COUNT * TOP_K
    slot_ids = lax.map(block_slots, expert_idx.reshape(GROUP_DEVS, TOK_DEV, TOP_K)).reshape(pair_count)
    flat_ids = expert_idx.reshape(pair_count)
    pair_pos = jnp.arange(pair_count)
    block_id = pair_pos // (TOK_DEV * TOP_K)
    tok_row = (pair_pos // TOP_K).astype(jnp.int32)
    per_expert = GROUP_DEVS * CAPACITY
    total_rows = NUM_EXPERTS * per_expert
    target = jnp.where(slot_ids < CAPACITY, flat_ids * per_expert + block_id * CAPACITY + slot_ids, total_rows)
    row_of = jnp.full((total_rows,), ROW_COUNT, jnp.int32).at[target].set(tok_row, mode='drop')
    gate_of = jnp.zeros((total_rows,), jnp.float32).at[target].set(gates.reshape(pair_count), mode='drop')
    padded = jnp.concatenate([tokens, jnp.zeros((1, MODEL_DIM), tokens.dtype)], axis=0)

    def expert_step(acc, stacked):
        wg_one, wu_one, wd_one, rows_one, gate_one = stacked
        picked = padded[rows_one]
        act_a = jnp.dot(picked, wg_one, preferred_element_type=jnp.float32)
        act_b = jnp.dot(picked, wu_one, preferred_element_type=jnp.float32)
        hidden = (jax.nn.silu(act_a) * act_b).astype(jnp.bfloat16)
        expert_out = jnp.dot(hidden, wd_one, preferred_element_type=jnp.float32).astype(jnp.bfloat16)
        acc = acc.at[rows_one].add(gate_one[:, None] * expert_out.astype(jnp.float32), mode='drop')
        return acc, None

    acc_init = jnp.zeros((ROW_COUNT, MODEL_DIM), jnp.float32)
    acc, unused = lax.scan(expert_step, acc_init, (w_gate, w_up, w_down, row_of.reshape(NUM_EXPERTS, per_expert), gate_of.reshape(NUM_EXPERTS, per_expert)))
    return (tokens.astype(jnp.float32) + acc).astype(jnp.bfloat16)
```

```python
import functools

import jax
import jax.numpy as jnp
from jax import lax
from jax.experimental import pallas as pl
from jax.experimental.pallas import tpu as pltpu
from jax.sharding import PartitionSpec as P

F32 = jnp.float32
BF16 = jnp.bfloat16
VMEM_LIMIT = 60 * 1024 * 1024


def expert_rows(idx_t, n_exp):
    tok = idx_t.shape[1]
    eid = lax.broadcasted_iota(jnp.int32, (n_exp, tok), 0)
    hit = jnp.zeros((n_exp, tok), F32)
    for j in range(idx_t.shape[0]):
        hit = jnp.where(idx_t[j:j + 1, :] == eid, 1.0, hit)
    return hit, eid


def slot_keys(hit):
    tok = hit.shape[1]
    src = lax.broadcasted_iota(jnp.int32, (tok, tok), 0)
    dst = lax.broadcasted_iota(jnp.int32, (tok, tok), 1)
    earlier = jnp.where(src < dst, 1.0, 0.0).astype(BF16)
    before = jnp.dot(hit.astype(BF16), earlier, preferred_element_type=F32)
    return jnp.where(hit > 0.5, before, -1.0)


def send_kernel(base, width, group, idx_ref, tok_ref, out_ref, key_ref):
    @pl.when(pl.program_id(0) == 0)
    def _():
        hit, _ = expert_rows(idx_ref[...], key_ref.shape[0])
        key_ref[...] = slot_keys(hit)

    keys = key_ref[pl.ds(pl.program_id(0) * group, group), :]
    slot = lax.broadcasted_iota(jnp.int32, (width, keys.shape[1]), 0).astype(F32) + float(base)
    pick = [jnp.where(keys[g:g + 1, :] == slot, 1.0, 0.0) for g in range(group)]
    pick = jnp.concatenate(pick, axis=0).astype(BF16)
    out_ref[...] = jnp.dot(pick, tok_ref[...], preferred_element_type=F32).astype(BF16)


def build_send(idx_t, tokens, n_exp, base, width):
    tok, dim = tokens.shape
    group = 8
    rows = n_exp * width
    return pl.pallas_call(
        functools.partial(send_kernel, base, width, group),
        grid=(n_exp // group,),
        out_shape=jax.ShapeDtypeStruct((rows, dim), BF16),
        in_specs=[pl.BlockSpec((idx_t.shape[0], tok), lambda i: (0, 0)), pl.BlockSpec((tok, dim), lambda i: (0, 0))],
        out_specs=pl.BlockSpec((group * width, dim), lambda i: (i, 0)),
        scratch_shapes=[pltpu.VMEM((n_exp, tok), F32)],
        compiler_params=pltpu.CompilerParams(dimension_semantics=("arbitrary",), vmem_limit_bytes=VMEM_LIMIT),
        cost_estimate=pl.CostEstimate(flops=2 * rows * tok * dim, bytes_accessed=2 * rows * dim, transcendentals=0),
        name="build_send",
    )(idx_t, tokens)


def mix_weight_kernel(base, width, idx_ref, gate_ref, out_ref):
    tok = idx_ref.shape[1]
    rows = out_ref.shape[1]
    n_exp = rows // width
    idx_t, gate_t = idx_ref[...], gate_ref[...]
    hit, eid = expert_rows(idx_t, n_exp)
    key = slot_keys(hit).astype(BF16)
    gate = jnp.zeros((n_exp, tok), F32)
    for j in range(idx_t.shape[0]):
        gate = jnp.where(idx_t[j:j + 1, :] == eid, gate_t[j:j + 1, :], gate)
    col = lax.broadcasted_iota(jnp.int32, (n_exp, rows), 1)
    own = lax.broadcasted_iota(jnp.int32, (n_exp, rows), 0) * width
    spread = jnp.where((col >= own) & (col < own + width), 1.0, 0.0).astype(BF16)
    slot = jnp.sum(jnp.where((col >= own) & (col < own + width), (col - own).astype(F32), 0.0), axis=0, keepdims=True)
    turn = functools.partial(lax.dot_general, dimension_numbers=(((0,), (0,)), ((), ())), preferred_element_type=F32)
    mine = turn(key, spread) == slot + float(base)
    rest = gate
    for part in range(3):
        piece = rest.astype(BF16)
        rest = rest - piece.astype(F32)
        out_ref[part * tok:(part + 1) * tok, :] = jnp.where(mine, turn(piece, spread), 0.0).astype(BF16)


def build_mix(idx_t, gates_t, n_exp, base, width):
    tok = idx_t.shape[1]
    return pl.pallas_call(
        functools.partial(mix_weight_kernel, base, width),
        out_shape=jax.ShapeDtypeStruct((3 * tok, n_exp * width), BF16),
        compiler_params=pltpu.CompilerParams(vmem_limit_bytes=VMEM_LIMIT),
        cost_estimate=pl.CostEstimate(flops=8 * tok * n_exp * n_exp * width, bytes_accessed=6 * tok * n_exp * width, transcendentals=0),
        name="build_mix",
    )(idx_t, gates_t)


def ffn_kernel(x_ref, g0, g1, u0, u1, d0, d1, out_ref, wgu, wd, sems):
    half, ffn = g0.shape

    @pl.when(pl.program_id(0) == 0)
    def _():
        me = lax.axis_index('fsdp')
        copies = []
        for other, (g, u, d) in enumerate(((g0, u0, d0), (g1, u1, d1))):
            pos = me if other == 0 else 1 - me
            at = pl.ds(pl.multiple_of(pos * half, half), half)
            copies.append(pltpu.make_async_copy(g, wgu.at[at, pl.ds(0, ffn)], sems.at[other, 0]))
            copies.append(pltpu.make_async_copy(u, wgu.at[at, pl.ds(ffn, ffn)], sems.at[other, 1]))
            copies.append(pltpu.make_async_copy(d, wd.at[:, at], sems.at[other, 2]))
        for c in copies:
            c.start()
        for c in copies:
            c.wait()

    both = jnp.dot(x_ref[...], wgu[...], preferred_element_type=F32)
    act_a, act_b = both[:, :ffn], both[:, ffn:]
    hidden = (act_a * jax.nn.sigmoid(act_a) * act_b).astype(BF16)
    out_ref[...] = jnp.dot(hidden, wd[...], preferred_element_type=F32).astype(BF16)


def ffn(x, own, other):
    rows, dim = x.shape
    half, width = own[0].shape
    block = min(512, rows)
    any_spec = pl.BlockSpec(memory_space=pl.ANY)
    return pl.pallas_call(
        ffn_kernel,
        grid=(rows // block,),
        out_shape=jax.ShapeDtypeStruct((rows, dim), BF16),
        in_specs=[pl.BlockSpec((block, dim), lambda i: (i, 0))] + [any_spec] * 6,
        out_specs=pl.BlockSpec((block, dim), lambda i: (i, 0)),
        scratch_shapes=[pltpu.VMEM((dim, 2 * width), BF16), pltpu.VMEM((width, dim), BF16), pltpu.SemaphoreType.DMA((2, 3))],
        compiler_params=pltpu.CompilerParams(dimension_semantics=("arbitrary",), vmem_limit_bytes=VMEM_LIMIT),
        cost_estimate=pl.CostEstimate(flops=6 * rows * dim * width, bytes_accessed=4 * rows * dim + 6 * dim * width, transcendentals=rows * width),
        name="ffn",
    )(x, own[0], other[0], own[1], other[1], own[2], other[2])


def mix_kernel(w_ref, back_ref, base_ref, out_ref):
    tok = base_ref.shape[0]
    parts = jnp.dot(w_ref[...], back_ref[...], preferred_element_type=F32)
    total = base_ref[...].astype(F32) + (parts[:tok] + parts[tok:2 * tok] + parts[2 * tok:])
    out_ref[...] = total.astype(out_ref.dtype)


def mix(weights, back, base, dtype):
    tok, dim = base.shape
    rows = back.shape[0]
    block = min(512, dim)
    return pl.pallas_call(
        mix_kernel,
        grid=(dim // block,),
        out_shape=jax.ShapeDtypeStruct((tok, dim), dtype),
        in_specs=[pl.BlockSpec(weights.shape, lambda i: (0, 0)), pl.BlockSpec((rows, block), lambda i: (0, i)), pl.BlockSpec((tok, block), lambda i: (0, i))],
        out_specs=pl.BlockSpec((tok, block), lambda i: (0, i)),
        compiler_params=pltpu.CompilerParams(dimension_semantics=("arbitrary",), vmem_limit_bytes=VMEM_LIMIT),
        cost_estimate=pl.CostEstimate(flops=6 * tok * rows * dim, bytes_accessed=2 * rows * dim, transcendentals=0),
        name="mix",
    )(weights, back, base)


def solution(mesh):
    ep_size = mesh.shape['ep']
    row_spec = P(('rep', 'ep', 'fsdp'), None)
    swap = [(0, 1), (1, 0)]

    def device_step(tokens, expert_idx, gates, w_gate, w_up, w_down):
        tok_count, top_k = expert_idx.shape
        dim = tokens.shape[1]
        n_exp = ep_size
        capacity = (2 * tok_count * top_k + n_exp - 1) // n_exp
        width = capacity // 2
        own = (w_gate[0], w_up[0], w_down[0])
        other = tuple(lax.ppermute(w, 'fsdp', swap) for w in own)
        idx_t, gates_t = expert_idx.T, gates.T

        send_a = build_send(idx_t, tokens, n_exp, 0, width)
        send_b = build_send(idx_t, tokens, n_exp, width, width)

        def exchange(x):
            return lax.all_to_all(x.reshape(n_exp, width, dim), 'ep', 0, 0, tiled=True).reshape(n_exp * width, dim)

        in_a = exchange(send_a)
        in_b = exchange(send_b)
        mix_a = build_mix(idx_t, gates_t, n_exp, 0, width)
        mix_b = build_mix(idx_t, gates_t, n_exp, width, width)
        out_a = ffn(in_a, own, other)
        back_a = exchange(out_a)
        out_b = ffn(in_b, own, other)
        back_b = exchange(out_b)
        part = mix(mix_a, back_a, tokens, F32)
        return mix(mix_b, back_b, part, BF16)

    return jax.shard_map(device_step, mesh=mesh, in_specs=(row_spec, row_spec, row_spec, P('ep', 'fsdp', None), P('ep', 'fsdp', None), P('ep', None, 'fsdp')), out_specs=row_spec, check_vma=False)
```

```python
import functools

import jax
import jax.numpy as jnp
from jax import lax
from jax.experimental import pallas as pl
from jax.experimental.pallas import tpu as pltpu
from jax.sharding import PartitionSpec as P

F32 = jnp.float32
BF16 = jnp.bfloat16
MESH = pl.DeviceIdType.MESH
SIDE = 4
STRIDE = (16, 4, 1)
N_EXP = 64
GROUPS, PER = 8, 8
RING = 4


def hits(idx_t, eid):
    hit = jnp.zeros((eid.shape[0], idx_t.shape[1]), F32)
    for j in range(6):
        hit = jnp.where(idx_t[j:j + 1, :] == eid, 1.0, hit)
    return hit


def slot_keys(hit, earlier):
    before = jnp.dot(hit.astype(BF16), earlier, preferred_element_type=F32)
    return jnp.where(hit > 0.5, before, -1.0)


def offset(g, i):
    dz = i // 2
    dy = (i % 2) * 2 + lax.rem(g, 2)
    dx = lax.rem(dz + dy + lax.div(g, 2), SIDE)
    return dz, dy, dx


def layer_kernel(cap, cuts, idx_ref, gate_ref, tok_ref, wg, wu, wd, out_ref, recv, back,
                 wgu, wdn, toks_z, toks_y, toks_x, idx_all, mixw, acc,
                 ag_send, ag_recv, ix_send, ix_recv, d_send, d_recv, w_loc, w_send, w_recv, c_send, c_recv):
    tok, dim = tok_ref.shape
    half, ffn = wg.shape
    rows = PER * cap
    me = lax.axis_index('ep')
    core = lax.axis_index('fsdp')
    pos = (lax.div(me, 16), lax.rem(lax.div(me, 4), 4), lax.rem(me, 4))
    gathered = (toks_z, toks_y, toks_x)

    def shifted(a, k):
        return me + (lax.rem(pos[a] + k, SIDE) - pos[a]) * STRIDE[a]

    def ag_copies(a, k):
        dev = {'ep': shifted(a, k)}
        lo, hi = cuts[a], cuts[a + 1]
        yield pltpu.make_async_remote_copy(src_ref=idx_ref, dst_ref=idx_all.at[a, k - 1], send_sem=ix_send.at[a, k - 1],
                                           recv_sem=ix_recv.at[a, k - 1], device_id=dev, device_id_type=MESH)
        yield pltpu.make_async_remote_copy(src_ref=tok_ref.at[:, pl.ds(lo, hi - lo)], dst_ref=gathered[a].at[k - 1],
                                           send_sem=ag_send.at[a, k - 1], recv_sem=ag_recv.at[a, k - 1],
                                           device_id=dev, device_id_type=MESH)

    for k in (2, 1, 3):
        for a in range(3):
            for c in ag_copies(a, k):
                c.start()

    at = pl.ds(pl.multiple_of(core * half, half), half)
    spots = ((wg, wgu.at[at, pl.ds(0, ffn)]), (wu, wgu.at[at, pl.ds(ffn, ffn)]), (wd, wdn.at[:, at]))
    w_copies = []
    for n, (src, dst) in enumerate(spots):
        w_copies.append(pltpu.make_async_copy(src, dst, w_loc.at[n]))
        w_copies.append(pltpu.make_async_remote_copy(src_ref=src, dst_ref=dst, send_sem=w_send.at[n], recv_sem=w_recv.at[n],
                                                     device_id={'fsdp': 1 - core}, device_id_type=MESH))
    for c in w_copies:
        c.start()

    before = lax.broadcasted_iota(jnp.int32, (tok, tok), 0)
    after = lax.broadcasted_iota(jnp.int32, (tok, tok), 1)
    earlier = jnp.where(before < after, 1.0, 0.0).astype(BF16)
    slot = lax.broadcasted_iota(jnp.int32, (cap, tok), 0).astype(F32)

    def plane_ids(a):
        q = lax.broadcasted_iota(jnp.int32, (16, 1), 0)
        u, v = q >> 2, q & 3
        others = [b for b in range(3) if b != a]
        first = ((pos[others[0]] + u) & 3) * STRIDE[others[0]]
        second = ((pos[others[1]] + v) & 3) * STRIDE[others[1]]
        return first + second + pos[a] * STRIDE[a]

    def place(a, lo, hi):
        spot = [slice(None) if b == a else pos[b] for b in range(3)]
        return recv.at[spot[0], spot[1], spot[2], :, pl.ds(lo, hi - lo)]

    def plane_copies(a, stage):
        lo, hi = cuts[a], cuts[a + 1]
        others = [b for b in range(3) if b != a]
        yield pltpu.make_async_copy(stage.at[0], place(a, lo, hi), d_send.at[a, 0])
        for q in (10, 5, 15, 7, 13, 2, 8, 6, 9, 11, 14, 1, 4, 3, 12):
            dev = me
            for b, step in zip(others, (q // 4, q % 4)):
                dev = dev + (lax.rem(pos[b] + step, SIDE) - pos[b]) * STRIDE[b]
            yield pltpu.make_async_remote_copy(src_ref=stage.at[q], dst_ref=place(a, lo, hi), send_sem=d_send.at[a, q],
                                               recv_sem=d_recv.at[a, q], device_id={'ep': dev}, device_id_type=MESH)

    def dispatch(stage_z, stage_y, stage_x):
        stages = (stage_z, stage_y, stage_x)

        def pick(a, k):
            lo, hi = cuts[a], cuts[a + 1]
            if k == 0:
                ids, block = idx_ref[...], tok_ref[:, lo:hi]
            else:
                for c in ag_copies(a, k):
                    c.wait_recv()
                ids, block = idx_all[a, k - 1], gathered[a][k - 1]
            key = slot_keys(hits(ids, plane_ids(a)), earlier)
            sel = [jnp.where(key[q:q + 1, :] == slot, 1.0, 0.0) for q in range(16)]
            sel = jnp.concatenate(sel, axis=0).astype(BF16)
            got = jnp.dot(sel, block, preferred_element_type=F32).astype(BF16)
            line = lax.rem(pos[a] + SIDE - k, SIDE)
            for q in range(16):
                stages[a][q, line] = got[q * cap:(q + 1) * cap]

        for a in range(3):
            pick(a, 0)
        for a in range(3):
            for k in (1, 3, 2):
                pick(a, k)
            for c in plane_copies(a, stages[a]):
                c.start()
        for a in range(3):
            for k in (2, 1, 3):
                for c in ag_copies(a, k):
                    c.wait_send()
        build_mix()
        for c in w_copies:
            c.wait()
        for a in range(3):
            for n, c in enumerate(plane_copies(a, stages[a])):
                if n == 0:
                    c.wait()
                else:
                    c.wait_recv()
                    c.wait_send()

    def build_mix():
        idx_t, gate_t = idx_ref[...], gate_ref[...]
        eid = lax.broadcasted_iota(jnp.int32, (N_EXP, tok), 0)
        key = slot_keys(hits(idx_t, eid), earlier).astype(BF16)
        gate = jnp.zeros((N_EXP, tok), F32)
        for j in range(6):
            gate = jnp.where(idx_t[j:j + 1, :] == eid, gate_t[j:j + 1, :], gate)
        pieces = []
        left = gate
        for part in range(3):
            pieces.append(left.astype(BF16))
            left = left - pieces[-1].astype(F32)
        turn = functools.partial(lax.dot_general, dimension_numbers=(((0,), (0,)), ((), ())), preferred_element_type=F32)
        col = lax.broadcasted_iota(jnp.int32, (N_EXP, rows), 1)
        row = lax.broadcasted_iota(jnp.int32, (N_EXP, rows), 0)
        nth = jnp.zeros((N_EXP, rows), jnp.int32)
        for n in range(1, PER):
            nth = nth + jnp.where(col >= n * cap, 1, 0)
        want = (col - nth * cap)[0:1].astype(F32)
        dz = nth >> 1

        @pl.loop(0, GROUPS)
        def _(g):
            dy = (nth & 1) * 2 + lax.rem(g, 2)
            dx = (dz + dy + lax.div(g, 2)) & 3
            exp = ((pos[0] - dz) & 3) * 16 + ((pos[1] - dy) & 3) * 4 + ((pos[2] - dx) & 3)
            spread = jnp.where(exp == row, 1.0, 0.0).astype(BF16)
            mine = turn(key, spread) == want
            span = pl.ds(pl.multiple_of(g * rows, 128), rows)
            for part in range(3):
                mixw[part * tok:(part + 1) * tok, span] = jnp.where(mine, turn(pieces[part], spread), 0.0).astype(BF16)

    stage_types = [pltpu.VMEM((16, SIDE, cap, cuts[a + 1] - cuts[a]), BF16) for a in range(3)]
    pl.run_scoped(dispatch, *stage_types)

    def work(xbuf, outs, land, x_sem, m_sem):
        def loads(g, do):
            for i in range(PER):
                dz, dy, dx = offset(g, i)
                src = recv.at[lax.rem(pos[0] + dz, SIDE), lax.rem(pos[1] + dy, SIDE), lax.rem(pos[2] + dx, SIDE)]
                pltpu.make_async_copy(src, xbuf.at[lax.rem(g, 2), pl.ds(i * cap, cap)], x_sem.at[lax.rem(g, 2)]).start()

        def sends(g):
            ring = lax.rem(g, RING)
            for i in range(PER):
                dz, dy, dx = offset(g, i)
                dev = lax.rem(pos[0] + dz, SIDE) * 16 + lax.rem(pos[1] + dy, SIDE) * 4 + lax.rem(pos[2] + dx, SIDE)
                span = pl.ds(i * cap, cap)

                def far():
                    pltpu.make_async_remote_copy(src_ref=outs.at[ring, span], dst_ref=back.at[g, span], send_sem=c_send.at[ring],
                                                 recv_sem=c_recv.at[g], device_id={'ep': dev}, device_id_type=MESH).start()

                if i > 0:
                    far()
                else:
                    pl.when(g > 0)(far)

                    @pl.when(g == 0)
                    def _():
                        pltpu.make_async_copy(outs.at[ring, span], back.at[g, span], c_send.at[ring]).start()

        def drain(ring):
            pltpu.make_async_copy(outs.at[ring], outs.at[ring], c_send.at[ring]).wait()

        loads(0, None)

        @pl.loop(0, GROUPS)
        def _(g):
            now = lax.rem(g, 2)
            pltpu.make_async_copy(xbuf.at[now], xbuf.at[now], x_sem.at[now]).wait()

            @pl.when(g < GROUPS - 1)
            def _():
                loads(g + 1, None)

            @pl.when(g >= RING)
            def _():
                drain(lax.rem(g, RING))

            both = jnp.dot(xbuf[now], wgu[...], preferred_element_type=F32)
            act_a, act_b = both[:, :ffn], both[:, ffn:]
            hidden = (act_a * jax.nn.sigmoid(act_a) * act_b).astype(BF16)
            outs[lax.rem(g, RING)] = jnp.dot(hidden, wdn[...], preferred_element_type=F32).astype(BF16)
            sends(g)

        for ring in range(RING):
            drain(ring)
        acc[...] = tok_ref[...].astype(F32)

        @pl.loop(0, GROUPS // 2)
        def _(r):
            for s in range(2):
                g = 2 * r + s

                @pl.when(g == 0)
                def _():
                    part = back.at[0, pl.ds(cap, rows - cap)]
                    pltpu.make_async_copy(part, part, c_recv.at[0]).wait()

                @pl.when(g > 0)
                def _():
                    pltpu.make_async_copy(back.at[g], back.at[g], c_recv.at[g]).wait()

            pltpu.make_async_copy(back.at[pl.ds(2 * r, 2)], land, m_sem).start()
            pltpu.make_async_copy(back.at[pl.ds(2 * r, 2)], land, m_sem).wait()
            w = mixw[:, pl.ds(pl.multiple_of(r * 2 * rows, 128), 2 * rows)]
            for n in range(0, dim, 512):
                block = land[:, :, n:n + 512].reshape(2 * rows, 512)
                parts = jnp.dot(w, block, preferred_element_type=F32)
                acc[:, n:n + 512] += parts[:tok] + parts[tok:2 * tok] + parts[2 * tok:]

        out_ref[...] = acc[...].astype(BF16)

    pl.run_scoped(work, pltpu.VMEM((2, rows, dim), BF16), pltpu.VMEM((RING, rows, dim), BF16), pltpu.VMEM((2, rows, dim), BF16),
                  pltpu.SemaphoreType.DMA((2,)), pltpu.SemaphoreType.DMA)


def solution(mesh):
    row_spec = P(('rep', 'ep', 'fsdp'), None)

    def device_step(tokens, expert_idx, gates, w_gate, w_up, w_down):
        tok, top_k = expert_idx.shape
        dim = tokens.shape[1]
        half, width = w_gate.shape[1:]
        cap = (2 * tok * top_k + N_EXP - 1) // N_EXP
        cuts = (0, 640, 1280, dim)
        rows = PER * cap
        idx_t = jnp.pad(expert_idx.T, ((0, 8 - top_k), (0, 0)))
        gate_t = gates.T
        vmem = pl.BlockSpec(memory_space=pltpu.VMEM)
        hbm = pl.BlockSpec(memory_space=pl.ANY)
        sem = pltpu.SemaphoreType.DMA
        out, _, _ = pl.pallas_call(
            functools.partial(layer_kernel, cap, cuts),
            out_shape=(jax.ShapeDtypeStruct((tok, dim), BF16), jax.ShapeDtypeStruct((SIDE, SIDE, SIDE, cap, dim), BF16),
                       jax.ShapeDtypeStruct((GROUPS, rows, dim), BF16)),
            in_specs=[vmem, vmem, vmem, hbm, hbm, hbm],
            out_specs=(vmem, hbm, hbm),
            scratch_shapes=[pltpu.VMEM((dim, 2 * width), BF16), pltpu.VMEM((width, dim), BF16)]
            + [pltpu.VMEM((3, tok, cuts[a + 1] - cuts[a]), BF16) for a in range(3)]
            + [pltpu.VMEM((3, 3, 8, tok), jnp.int32), pltpu.VMEM((3 * tok, N_EXP * cap), BF16), pltpu.VMEM((tok, dim), F32),
               sem((3, 3)), sem((3, 3)), sem((3, 3)), sem((3, 3)), sem((3, 16)), sem((3, 16)), sem((3,)), sem((3,)), sem((3,)),
               sem((RING,)), sem((GROUPS,))],
            compiler_params=pltpu.CompilerParams(has_side_effects=True, vmem_limit_bytes=63 * 1024 * 1024),
            name="moe_layer",
        )(idx_t, gate_t, tokens, w_gate[0], w_up[0], w_down[0])
        return out

    return jax.shard_map(device_step, mesh=mesh, in_specs=(row_spec, row_spec, row_spec, P('ep', 'fsdp', None), P('ep', 'fsdp', None), P('ep', None, 'fsdp')), out_specs=row_spec, check_vma=False)
```

```python
import functools

import jax
import jax.numpy as jnp
from jax import lax
from jax.experimental import pallas as pl
from jax.experimental.pallas import tpu as pltpu
from jax.sharding import PartitionSpec as P

F32 = jnp.float32
BF16 = jnp.bfloat16
MESH = pl.DeviceIdType.MESH
SIDE = 4
STRIDE = (16, 4, 1)
N_EXP = 64
GROUPS, PER = 8, 8
ROUTES = ((2, 1, 0), (1, 0, 2), (0, 2, 1))
RING = 4


def hits(idx_t, eid):
    hit = jnp.zeros((eid.shape[0], idx_t.shape[1]), F32)
    for j in range(6):
        hit = jnp.where(idx_t[j:j + 1, :] == eid, 1.0, hit)
    return hit


def slot_keys(hit, earlier):
    before = jnp.dot(hit.astype(BF16), earlier, preferred_element_type=F32)
    return jnp.where(hit > 0.5, before, -1.0)


def offset(g, i):
    dz, b = i // 2, i % 2
    lean = 2 * b + lax.rem(g, 2)
    return dz, lax.rem(dz + lean, SIDE), lax.rem(lean + lax.div(g, 2) + SIDE - dz, SIDE)


def moved(d):
    return (d + SIDE - 1) // SIDE if isinstance(d, int) else lax.div(d + SIDE - 1, SIDE)


def if_moves(d, far, near=None):
    if isinstance(d, int):
        (far if d else near or (lambda: None))()
        return
    pl.when(d > 0)(far)
    if near is not None:
        pl.when(d == 0)(near)


def layer_kernel(cap, cuts, idx_ref, gate_ref, tok_ref, wg, wu, wd, out_ref, recv, back,
                 wgu, wdn, toks_z, toks_y, toks_x, idx_all, mixw, acc,
                 ag_send, ag_recv, ix_send, ix_recv, d_send, d_recv, w_loc, w_send, w_recv, c_send, c_keep, c_recv, r_send):
    tok, dim = tok_ref.shape
    half, ffn = wg.shape
    rows = PER * cap
    me = lax.axis_index('ep')
    core = lax.axis_index('fsdp')
    pos = (lax.div(me, 16), lax.rem(lax.div(me, 4), 4), lax.rem(me, 4))
    gathered = (toks_z, toks_y, toks_x)

    def shifted(a, k):
        return me + (lax.rem(pos[a] + k, SIDE) - pos[a]) * STRIDE[a]

    def ag_copies(a, k):
        dev = {'ep': shifted(a, k)}
        lo, hi = cuts[a], cuts[a + 1]
        yield pltpu.make_async_remote_copy(src_ref=idx_ref, dst_ref=idx_all.at[a, k - 1], send_sem=ix_send.at[a, k - 1],
                                           recv_sem=ix_recv.at[a, k - 1], device_id=dev, device_id_type=MESH)
        yield pltpu.make_async_remote_copy(src_ref=tok_ref.at[:, pl.ds(lo, hi - lo)], dst_ref=gathered[a].at[k - 1],
                                           send_sem=ag_send.at[a, k - 1], recv_sem=ag_recv.at[a, k - 1],
                                           device_id=dev, device_id_type=MESH)

    for k in (2, 1, 3):
        for a in range(3):
            for c in ag_copies(a, k):
                c.start()

    at = pl.ds(pl.multiple_of(core * half, half), half)
    spots = ((wg, wgu.at[at, pl.ds(0, ffn)]), (wu, wgu.at[at, pl.ds(ffn, ffn)]), (wd, wdn.at[:, at]))
    w_copies = []
    for n, (src, dst) in enumerate(spots):
        w_copies.append(pltpu.make_async_copy(src, dst, w_loc.at[n]))
        w_copies.append(pltpu.make_async_remote_copy(src_ref=src, dst_ref=dst, send_sem=w_send.at[n], recv_sem=w_recv.at[n],
                                                     device_id={'fsdp': 1 - core}, device_id_type=MESH))
    before = lax.broadcasted_iota(jnp.int32, (tok, tok), 0)
    after = lax.broadcasted_iota(jnp.int32, (tok, tok), 1)
    earlier = jnp.where(before < after, 1.0, 0.0).astype(BF16)
    slot = lax.broadcasted_iota(jnp.int32, (cap, tok), 0).astype(F32)

    def plane_ids(a):
        q = lax.broadcasted_iota(jnp.int32, (16, 1), 0)
        u, v = q >> 2, q & 3
        others = [b for b in range(3) if b != a]
        first = ((pos[others[0]] + u) & 3) * STRIDE[others[0]]
        second = ((pos[others[1]] + v) & 3) * STRIDE[others[1]]
        return first + second + pos[a] * STRIDE[a]

    def place(a, lo, hi):
        spot = [slice(None) if b == a else pos[b] for b in range(3)]
        return recv.at[spot[0], spot[1], spot[2], :, pl.ds(lo, hi - lo)]

    def plane_copies(a, stage):
        lo, hi = cuts[a], cuts[a + 1]
        others = [b for b in range(3) if b != a]
        yield pltpu.make_async_copy(stage.at[0], place(a, lo, hi), d_send.at[a, 0])
        for q in (10, 5, 15, 7, 13, 2, 8, 6, 9, 11, 14, 1, 4, 3, 12):
            dev = me
            for b, step in zip(others, (q // 4, q % 4)):
                dev = dev + (lax.rem(pos[b] + step, SIDE) - pos[b]) * STRIDE[b]
            yield pltpu.make_async_remote_copy(src_ref=stage.at[q], dst_ref=place(a, lo, hi), send_sem=d_send.at[a, q],
                                               recv_sem=d_recv.at[a, q], device_id={'ep': dev}, device_id_type=MESH)

    def dispatch(stage_z, stage_y, stage_x):
        stages = (stage_z, stage_y, stage_x)

        def pick(a, k):
            lo, hi = cuts[a], cuts[a + 1]
            if k == 0:
                ids, block = idx_ref[...], tok_ref[:, lo:hi]
            else:
                for c in ag_copies(a, k):
                    c.wait_recv()
                ids, block = idx_all[a, k - 1], gathered[a][k - 1]
            key = slot_keys(hits(ids, plane_ids(a)), earlier)
            sel = [jnp.where(key[q:q + 1, :] == slot, 1.0, 0.0) for q in range(16)]
            sel = jnp.concatenate(sel, axis=0).astype(BF16)
            got = jnp.dot(sel, block, preferred_element_type=F32).astype(BF16)
            line = lax.rem(pos[a] + SIDE - k, SIDE)
            for q in range(16):
                stages[a][q, line] = got[q * cap:(q + 1) * cap]

        for k in (0, 1, 3, 2):
            for a in range(3):
                pick(a, k)
        for trio in zip(*(plane_copies(a, stages[a]) for a in range(3))):
            for c in trio:
                c.start()
        for c in w_copies:
            c.start()
        for a in range(3):
            for k in (2, 1, 3):
                for c in ag_copies(a, k):
                    c.wait_send()
        build_mix()
        for c in w_copies:
            c.wait()
        for a in range(3):
            for n, c in enumerate(plane_copies(a, stages[a])):
                if n == 0:
                    c.wait()
                else:
                    c.wait_recv()
                    c.wait_send()

    def build_mix():
        idx_t, gate_t = idx_ref[...], gate_ref[...]
        eid = lax.broadcasted_iota(jnp.int32, (N_EXP, tok), 0)
        key = slot_keys(hits(idx_t, eid), earlier).astype(BF16)
        gate = jnp.zeros((N_EXP, tok), F32)
        for j in range(6):
            gate = jnp.where(idx_t[j:j + 1, :] == eid, gate_t[j:j + 1, :], gate)
        pieces = []
        left = gate
        for part in range(3):
            pieces.append(left.astype(BF16))
            left = left - pieces[-1].astype(F32)
        turn = functools.partial(lax.dot_general, dimension_numbers=(((0,), (0,)), ((), ())), preferred_element_type=F32)
        col = lax.broadcasted_iota(jnp.int32, (N_EXP, rows), 1)
        row = lax.broadcasted_iota(jnp.int32, (N_EXP, rows), 0)
        nth = jnp.zeros((N_EXP, rows), jnp.int32)
        for n in range(1, PER):
            nth = nth + jnp.where(col >= n * cap, 1, 0)
        want = (col - nth * cap)[0:1].astype(F32)
        dz = nth >> 1

        @pl.loop(0, GROUPS)
        def _(g):
            lean = (nth & 1) * 2 + lax.rem(g, 2)
            dy = (dz + lean) & 3
            dx = (lean + lax.div(g, 2) - dz) & 3
            exp = ((pos[0] - dz) & 3) * 16 + ((pos[1] - dy) & 3) * 4 + ((pos[2] - dx) & 3)
            spread = jnp.where(exp == row, 1.0, 0.0).astype(BF16)
            mine = turn(key, spread) == want
            span = pl.ds(pl.multiple_of(g * rows, 128), rows)
            for part in range(3):
                mixw[part * tok:(part + 1) * tok, span] = jnp.where(mine, turn(pieces[part], spread), 0.0).astype(BF16)

    stage_types = [pltpu.VMEM((16, SIDE, cap, cuts[a + 1] - cuts[a]), BF16) for a in range(3)]
    pl.run_scoped(dispatch, *stage_types)

    def work(xbuf, outs, land, x_sem, m_sem):
        def loads(g):
            for i in range(PER):
                dz, dy, dx = offset(g, i)
                src = recv.at[lax.rem(pos[0] + dz, SIDE), lax.rem(pos[1] + dy, SIDE), lax.rem(pos[2] + dx, SIDE)]
                pltpu.make_async_copy(src, xbuf.at[lax.rem(g, 2), pl.ds(i * cap, cap)], x_sem.at[lax.rem(g, 2)]).start()

        def block(i, p):
            return pl.ds(i * cap, cap), pl.ds(cuts[p], cuts[p + 1] - cuts[p])

        def hop(src, stage, g, i, p, d, send):
            axis = ROUTES[p][stage]
            return pltpu.make_async_remote_copy(
                src_ref=src, dst_ref=back.at[stage, g, *block(i, p)], send_sem=send, recv_sem=c_recv.at[stage, g],
                device_id={'ep': shifted(axis, d)}, device_id_type=MESH)

        def each(g):
            for i in range(PER):
                ds = offset(g, i)
                for p in range(3):
                    yield i, p, [ds[axis] for axis in ROUTES[p]]

        def first_hops(g):
            ring = lax.rem(g, RING)
            for i, p, d in each(g):
                src = outs.at[ring, *block(i, p)]
                if_moves(d[0], lambda: hop(src, 0, g, i, p, d[0], c_send.at[ring]).start(),
                         lambda: pltpu.make_async_copy(src, back.at[0, g, *block(i, p)], c_keep.at[g]).start())

        def second_hops(g):
            arrived(0, g)
            part = back.at[0, g, pl.ds(0, rows - far)]
            pltpu.make_async_copy(part, part, c_keep.at[g]).wait()
            for i, p, d in each(g):
                if_moves(d[1], lambda: hop(back.at[0, g, *block(i, p)], 1, g, i, p, d[1], r_send.at[0]).start())

        def third_hops(g):
            arrived(1, g)
            for i, p, d in each(g):
                if_moves(d[2], lambda: hop(back.at[moved(d[1]), g, *block(i, p)], 2, g, i, p, d[2], r_send.at[1]).start())

        def arrived(stage, g):
            part = back.at[stage, g, pl.ds(0, far)]
            pltpu.make_async_copy(part, part, c_recv.at[stage, g]).wait()

        def drain(ring):
            part = outs.at[ring, pl.ds(0, far)]
            pltpu.make_async_copy(part, part, c_send.at[ring]).wait()

        def experts(g):
            now = lax.rem(g, 2)
            pltpu.make_async_copy(xbuf.at[now], xbuf.at[now], x_sem.at[now]).wait()

            @pl.when(g < GROUPS - 1)
            def _():
                loads(g + 1)

            @pl.when(g >= RING)
            def _():
                drain(lax.rem(g, RING))

            both = jnp.dot(xbuf[now], wgu[...], preferred_element_type=F32)
            act_a, act_b = both[:, :ffn], both[:, ffn:]
            hidden = (act_a * jax.nn.sigmoid(act_a) * act_b).astype(BF16)
            outs[lax.rem(g, RING)] = jnp.dot(hidden, wdn[...], preferred_element_type=F32).astype(BF16)
            first_hops(g)

        def mix(g):
            arrived(2, g)
            for i, p, d in each(g):
                last = moved(d[2])
                stage = 2 * last + (1 - last) * moved(d[1])
                pltpu.make_async_copy(back.at[stage, g, *block(i, p)], land.at[block(i, p)], m_sem).start()
            pltpu.make_async_copy(land, land, m_sem).wait()
            w = mixw[:, pl.ds(pl.multiple_of(g * rows, 128), rows)]
            for n in range(0, dim, 512):
                parts = jnp.dot(w, land[:, n:n + 512], preferred_element_type=F32)
                acc[:, n:n + 512] += parts[:tok] + parts[tok:2 * tok] + parts[2 * tok:]

        far = rows // SIDE * (SIDE - 1)
        acc[...] = tok_ref[...].astype(F32)
        loads(0)

        @pl.loop(0, GROUPS + 3)
        def _(r):
            @pl.when(r < GROUPS)
            def _():
                experts(r)

            @pl.when((r >= 1) & (r < GROUPS + 1))
            def _():
                second_hops(r - 1)

            @pl.when((r >= 2) & (r < GROUPS + 2))
            def _():
                third_hops(r - 2)

            @pl.when(r >= 3)
            def _():
                mix(r - 3)

        out_ref[...] = acc[...].astype(BF16)
        for ring in range(RING):
            drain(ring)
        for n in range(2):
            part = back.at[0, :, pl.ds(0, far)]
            pltpu.make_async_copy(part, part, r_send.at[n]).wait()

    pl.run_scoped(work, pltpu.VMEM((2, rows, dim), BF16), pltpu.VMEM((RING, rows, dim), BF16), pltpu.VMEM((rows, dim), BF16),
                  pltpu.SemaphoreType.DMA((2,)), pltpu.SemaphoreType.DMA)


def solution(mesh):
    row_spec = P(('rep', 'ep', 'fsdp'), None)

    def device_step(tokens, expert_idx, gates, w_gate, w_up, w_down):
        tok, top_k = expert_idx.shape
        dim = tokens.shape[1]
        half, width = w_gate.shape[1:]
        cap = (2 * tok * top_k + N_EXP - 1) // N_EXP
        cuts = (0, 640, 1280, dim)
        rows = PER * cap
        idx_t = jnp.pad(expert_idx.T, ((0, 8 - top_k), (0, 0)))
        gate_t = gates.T
        vmem = pl.BlockSpec(memory_space=pltpu.VMEM)
        hbm = pl.BlockSpec(memory_space=pl.ANY)
        sem = pltpu.SemaphoreType.DMA
        out, _, _ = pl.pallas_call(
            functools.partial(layer_kernel, cap, cuts),
            out_shape=(jax.ShapeDtypeStruct((tok, dim), BF16), jax.ShapeDtypeStruct((SIDE, SIDE, SIDE, cap, dim), BF16),
                       jax.ShapeDtypeStruct((3, GROUPS, rows, dim), BF16)),
            in_specs=[vmem, vmem, vmem, hbm, hbm, hbm],
            out_specs=(vmem, hbm, hbm),
            scratch_shapes=[pltpu.VMEM((dim, 2 * width), BF16), pltpu.VMEM((width, dim), BF16)]
            + [pltpu.VMEM((3, tok, cuts[a + 1] - cuts[a]), BF16) for a in range(3)]
            + [pltpu.VMEM((3, 3, 8, tok), jnp.int32), pltpu.VMEM((3 * tok, N_EXP * cap), BF16), pltpu.VMEM((tok, dim), F32),
               sem((3, 3)), sem((3, 3)), sem((3, 3)), sem((3, 3)), sem((3, 16)), sem((3, 16)), sem((3,)), sem((3,)), sem((3,)),
               sem((RING,)), sem((GROUPS,)), sem((3, GROUPS)), sem((2,))],
            compiler_params=pltpu.CompilerParams(has_side_effects=True, vmem_limit_bytes=63 * 1024 * 1024),
            name="moe_layer",
        )(idx_t, gate_t, tokens, w_gate[0], w_up[0], w_down[0])
        return out

    return jax.shard_map(device_step, mesh=mesh, in_specs=(row_spec, row_spec, row_spec, P('ep', 'fsdp', None), P('ep', 'fsdp', None), P('ep', None, 'fsdp')), out_specs=row_spec, check_vma=False)
```

```python
import functools

import jax
import jax.numpy as jnp
from jax import lax
from jax.experimental import pallas as pl
from jax.experimental.pallas import tpu as pltpu
from jax.sharding import PartitionSpec as P

F32 = jnp.float32
BF16 = jnp.bfloat16
MESH = pl.DeviceIdType.MESH
SIDE = 4
STRIDE = (16, 4, 1)
N_EXP = 64
GROUPS, PER = 8, 8
ROUTES = ((2, 1, 0), (1, 0, 2), (0, 2, 1))
OUT_ROUTES = ((0, 1, 2), (1, 2, 0), (2, 0, 1))
LEAD = 2
RING = 4


def hits(idx_t, eid):
    hit = jnp.zeros((eid.shape[0], idx_t.shape[1]), F32)
    for j in range(6):
        hit = jnp.where(idx_t[j:j + 1, :] == eid, 1.0, hit)
    return hit


def slot_keys(hit, earlier):
    before = jnp.dot(hit.astype(BF16), earlier, preferred_element_type=F32)
    return jnp.where(hit > 0.5, before, -1.0)


def offset(g, i):
    dz, b = i // 2, i % 2
    lean = 2 * b + lax.rem(g, 2)
    return dz, lax.rem(dz + lean, SIDE), lax.rem(lean + lax.div(g, 2) + SIDE - dz, SIDE)


def moved(d):
    return (d + SIDE - 1) // SIDE if isinstance(d, int) else lax.div(d + SIDE - 1, SIDE)


def if_moves(d, far, near=None):
    if isinstance(d, int):
        (far if d else near or (lambda: None))()
        return
    pl.when(d > 0)(far)
    if near is not None:
        pl.when(d == 0)(near)


def layer_kernel(cap, cuts, idx_ref, gate_ref, tok_ref, wg, wu, wd, out_ref, inbox, back,
                 wgu, wdn, toks_z, toks_y, toks_x, idx_all, keys, mixw, acc, stage, xbuf, outs, land,
                 ag_send, ag_recv, ix_send, ix_recv, w_loc, w_send, w_recv,
                 d_send, d_keep, d_recv, d_relay, c_send, c_keep, c_recv, c_relay, x_sem, m_sem):
    tok, dim = tok_ref.shape
    half, ffn = wg.shape
    rows = PER * cap
    far = rows // SIDE * (SIDE - 1)
    me = lax.axis_index('ep')
    core = lax.axis_index('fsdp')
    pos = (lax.div(me, 16), lax.rem(lax.div(me, 4), 4), lax.rem(me, 4))
    gathered = (toks_z, toks_y, toks_x)

    def shifted(a, k):
        return me + (lax.rem(pos[a] + k, SIDE) - pos[a]) * STRIDE[a]

    def ag_copies(a, k):
        dev = {'ep': shifted(a, k)}
        lo, hi = cuts[a], cuts[a + 1]
        yield pltpu.make_async_remote_copy(src_ref=idx_ref, dst_ref=idx_all.at[a, k - 1], send_sem=ix_send.at[a, k - 1],
                                           recv_sem=ix_recv.at[a, k - 1], device_id=dev, device_id_type=MESH)
        yield pltpu.make_async_remote_copy(src_ref=tok_ref.at[:, pl.ds(lo, hi - lo)], dst_ref=gathered[a].at[k],
                                           send_sem=ag_send.at[a, k - 1], recv_sem=ag_recv.at[a, k - 1],
                                           device_id=dev, device_id_type=MESH)

    for k in (2, 1, 3):
        for a in range(3):
            for c in ag_copies(a, k):
                c.start()

    at = pl.ds(pl.multiple_of(core * half, half), half)
    spots = ((wg, wgu.at[at, pl.ds(0, ffn)]), (wu, wgu.at[at, pl.ds(ffn, ffn)]), (wd, wdn.at[:, at]))
    w_copies = []
    for n, (src, dst) in enumerate(spots):
        w_copies.append(pltpu.make_async_copy(src, dst, w_loc.at[n]))
        w_copies.append(pltpu.make_async_remote_copy(src_ref=src, dst_ref=dst, send_sem=w_send.at[n], recv_sem=w_recv.at[n],
                                                     device_id={'fsdp': 1 - core}, device_id_type=MESH))

    before = lax.broadcasted_iota(jnp.int32, (tok, tok), 0)
    after = lax.broadcasted_iota(jnp.int32, (tok, tok), 1)
    earlier = jnp.where(before < after, 1.0, 0.0).astype(BF16)
    slot = lax.broadcasted_iota(jnp.int32, (cap, tok), 0).astype(F32)

    def block(i, p):
        return pl.ds(i * cap, cap), pl.ds(cuts[p], cuts[p + 1] - cuts[p])

    def each(g, routes):
        for i in range(PER):
            ds = offset(g, i)
            for p in range(3):
                yield i, p, [ds[axis] for axis in routes[p]]

    def wait_rows(ref, n, sem):
        part = ref.at[pl.ds(0, n)]
        pltpu.make_async_copy(part, part, sem).wait()

    def plane_keys(a, k):
        q = lax.broadcasted_iota(jnp.int32, (16, 1), 0)
        _, b, c = OUT_ROUTES[a]
        eid = pos[a] * STRIDE[a] + ((pos[b] + (q >> 2)) & 3) * STRIDE[b] + ((pos[c] + (q & 3)) & 3) * STRIDE[c]
        ids = idx_ref[...] if k == 0 else idx_all[a, k - 1]
        keys[a, k] = slot_keys(hits(ids, eid), earlier)

    def back_of(d):
        return (SIDE - d) % SIDE if isinstance(d, int) else lax.rem(SIDE - d, SIDE)

    def pick(g):
        ring = lax.rem(g, RING)

        @pl.when(g >= RING)
        def _():
            wait_rows(stage.at[ring], far, d_send.at[ring])

        for i, p, d in each(g, OUT_ROUTES):
            lo, hi = cuts[p], cuts[p + 1]
            k = back_of(d[0])
            key = keys[p, k, pl.ds(back_of(d[1]) * 4 + back_of(d[2]), 1), :]
            sel = jnp.where(key == slot, 1.0, 0.0).astype(BF16)
            got = jnp.dot(sel, gathered[p][k], preferred_element_type=F32)
            stage[ring, i * cap:(i + 1) * cap, lo:hi] = got.astype(BF16)
        for i, p, d in each(g, OUT_ROUTES):
            src, dst = stage.at[ring, *block(i, p)], inbox.at[0, g, *block(i, p)]
            if_moves(d[1], lambda: pltpu.make_async_remote_copy(
                src_ref=src, dst_ref=dst, send_sem=d_send.at[ring], recv_sem=d_recv.at[0, g],
                device_id={'ep': shifted(OUT_ROUTES[p][1], back_of(d[1]))}, device_id_type=MESH).start(),
                lambda: pltpu.make_async_copy(src, dst, d_keep.at[g]).start())

    def forward(g):
        wait_rows(inbox.at[0, g], far, d_recv.at[0, g])
        wait_rows(inbox.at[0, g], rows - far, d_keep.at[g])
        for i, p, d in each(g, OUT_ROUTES):
            if_moves(d[2], lambda: pltpu.make_async_remote_copy(
                src_ref=inbox.at[0, g, *block(i, p)], dst_ref=inbox.at[1, g, *block(i, p)], send_sem=d_relay,
                recv_sem=d_recv.at[1, g], device_id={'ep': shifted(OUT_ROUTES[p][2], back_of(d[2]))}, device_id_type=MESH).start())

    def fetch(g):
        wait_rows(inbox.at[1, g], far, d_recv.at[1, g])
        for i, p, d in each(g, OUT_ROUTES):
            pltpu.make_async_copy(inbox.at[moved(d[2]), g, *block(i, p)], xbuf.at[block(i, p)], x_sem).start()

    def build_mix():
        idx_t, gate_t = idx_ref[...], gate_ref[...]
        eid = lax.broadcasted_iota(jnp.int32, (N_EXP, tok), 0)
        key = slot_keys(hits(idx_t, eid), earlier).astype(BF16)
        gate = jnp.zeros((N_EXP, tok), F32)
        for j in range(6):
            gate = jnp.where(idx_t[j:j + 1, :] == eid, gate_t[j:j + 1, :], gate)
        pieces = []
        left = gate
        for part in range(3):
            pieces.append(left.astype(BF16))
            left = left - pieces[-1].astype(F32)
        turn = functools.partial(lax.dot_general, dimension_numbers=(((0,), (0,)), ((), ())), preferred_element_type=F32)
        col = lax.broadcasted_iota(jnp.int32, (N_EXP, rows), 1)
        row = lax.broadcasted_iota(jnp.int32, (N_EXP, rows), 0)
        nth = jnp.zeros((N_EXP, rows), jnp.int32)
        for n in range(1, PER):
            nth = nth + jnp.where(col >= n * cap, 1, 0)
        want = (col - nth * cap)[0:1].astype(F32)
        dz = nth >> 1

        @pl.loop(0, GROUPS)
        def _(g):
            lean = (nth & 1) * 2 + lax.rem(g, 2)
            dy = (dz + lean) & 3
            dx = (lean + lax.div(g, 2) - dz) & 3
            exp = ((pos[0] - dz) & 3) * 16 + ((pos[1] - dy) & 3) * 4 + ((pos[2] - dx) & 3)
            spread = jnp.where(exp == row, 1.0, 0.0).astype(BF16)
            mine = turn(key, spread) == want
            span = pl.ds(pl.multiple_of(g * rows, 128), rows)
            for part in range(3):
                mixw[part * tok:(part + 1) * tok, span] = jnp.where(mine, turn(pieces[part], spread), 0.0).astype(BF16)

    def experts(g):
        ring = lax.rem(g, RING)
        pltpu.make_async_copy(xbuf, xbuf, x_sem).wait()

        @pl.when(g >= RING)
        def _():
            wait_rows(outs.at[ring], far, c_send.at[ring])

        both = jnp.dot(xbuf[...], wgu[...], preferred_element_type=F32)
        act_a, act_b = both[:, :ffn], both[:, ffn:]
        hidden = (act_a * jax.nn.sigmoid(act_a) * act_b).astype(BF16)
        outs[ring] = jnp.dot(hidden, wdn[...], preferred_element_type=F32).astype(BF16)
        for i, p, d in each(g, ROUTES):
            src = outs.at[ring, *block(i, p)]
            if_moves(d[0], lambda: hop(src, 0, g, i, p, d[0], c_send.at[ring]).start(),
                     lambda: pltpu.make_async_copy(src, back.at[0, g, *block(i, p)], c_keep.at[g]).start())

    def hop(src, leg, g, i, p, d, send):
        return pltpu.make_async_remote_copy(
            src_ref=src, dst_ref=back.at[leg, g, *block(i, p)], send_sem=send, recv_sem=c_recv.at[leg, g],
            device_id={'ep': shifted(ROUTES[p][leg], d)}, device_id_type=MESH)

    def second_hops(g):
        wait_rows(back.at[0, g], far, c_recv.at[0, g])
        wait_rows(back.at[0, g], rows - far, c_keep.at[g])
        for i, p, d in each(g, ROUTES):
            if_moves(d[1], lambda: hop(back.at[0, g, *block(i, p)], 1, g, i, p, d[1], c_relay.at[0]).start())

    def third_hops(g):
        wait_rows(back.at[1, g], far, c_recv.at[1, g])
        for i, p, d in each(g, ROUTES):
            if_moves(d[2], lambda: hop(back.at[moved(d[1]), g, *block(i, p)], 2, g, i, p, d[2], c_relay.at[1]).start())

    def mix(g):
        wait_rows(back.at[2, g], far, c_recv.at[2, g])
        for i, p, d in each(g, ROUTES):
            last = moved(d[2])
            leg = 2 * last + (1 - last) * moved(d[1])
            pltpu.make_async_copy(back.at[leg, g, *block(i, p)], land.at[block(i, p)], m_sem).start()
        pltpu.make_async_copy(land, land, m_sem).wait()
        w = mixw[:, pl.ds(pl.multiple_of(g * rows, 128), rows)]
        for n in range(0, dim, 512):
            parts = jnp.dot(w, land[:, n:n + 512], preferred_element_type=F32)
            acc[:, n:n + 512] += parts[:tok] + parts[tok:2 * tok] + parts[2 * tok:]

    acc[...] = tok_ref[...].astype(F32)
    for a in range(3):
        gathered[a][0] = tok_ref[:, cuts[a]:cuts[a + 1]]
        plane_keys(a, 0)
    for k in (1, 3, 2):
        for a in range(3):
            for c in ag_copies(a, k):
                c.wait_recv()
            plane_keys(a, k)
    for g in range(LEAD):
        pick(jnp.int32(g))
    for c in w_copies:
        c.start()
    build_mix()
    for a in range(3):
        for k in (2, 1, 3):
            for c in ag_copies(a, k):
                c.wait_send()

    def in_turn(r, lag, step):
        g = r - lag
        pl.when((g >= 0) & (g < GROUPS))(lambda: step(g))

    @pl.loop(0, GROUPS + 4)
    def _(r):
        @pl.when(r == 1)
        def _():
            for c in w_copies:
                c.wait()

        in_turn(r, 0, forward)
        in_turn(r, 1, fetch)
        pl.when(r + LEAD < GROUPS)(lambda: pick(r + LEAD))
        in_turn(r, 1, experts)
        in_turn(r, 2, second_hops)
        in_turn(r, 3, third_hops)
        in_turn(r, 4, mix)

    out_ref[...] = acc[...].astype(BF16)
    for ring in range(RING):
        wait_rows(stage.at[ring], far, d_send.at[ring])
        wait_rows(outs.at[ring], far, c_send.at[ring])
    for sem in (d_relay, c_relay.at[0], c_relay.at[1]):
        part = back.at[0, :, pl.ds(0, far)]
        pltpu.make_async_copy(part, part, sem).wait()


def solution(mesh):
    row_spec = P(('rep', 'ep', 'fsdp'), None)

    def device_step(tokens, expert_idx, gates, w_gate, w_up, w_down):
        tok, top_k = expert_idx.shape
        dim = tokens.shape[1]
        half, width = w_gate.shape[1:]
        cap = (2 * tok * top_k + N_EXP - 1) // N_EXP
        cuts = (0, 640, 1280, dim)
        rows = PER * cap
        idx_t = jnp.pad(expert_idx.T, ((0, 8 - top_k), (0, 0)))
        gate_t = gates.T
        vmem = pl.BlockSpec(memory_space=pltpu.VMEM)
        hbm = pl.BlockSpec(memory_space=pl.ANY)
        sem = pltpu.SemaphoreType.DMA
        out, _, _ = pl.pallas_call(
            functools.partial(layer_kernel, cap, cuts),
            out_shape=(jax.ShapeDtypeStruct((tok, dim), BF16), jax.ShapeDtypeStruct((2, GROUPS, rows, dim), BF16),
                       jax.ShapeDtypeStruct((3, GROUPS, rows, dim), BF16)),
            in_specs=[vmem, vmem, vmem, hbm, hbm, hbm],
            out_specs=(vmem, hbm, hbm),
            scratch_shapes=[pltpu.VMEM((dim, 2 * width), BF16), pltpu.VMEM((width, dim), BF16)]
            + [pltpu.VMEM((SIDE, tok, cuts[a + 1] - cuts[a]), BF16) for a in range(3)]
            + [pltpu.VMEM((3, 3, 8, tok), jnp.int32), pltpu.VMEM((3, SIDE, 16, tok), F32), pltpu.VMEM((3 * tok, N_EXP * cap), BF16),
               pltpu.VMEM((tok, dim), F32), pltpu.VMEM((RING, rows, dim), BF16), pltpu.VMEM((rows, dim), BF16),
               pltpu.VMEM((RING, rows, dim), BF16), pltpu.VMEM((rows, dim), BF16),
               sem((3, 3)), sem((3, 3)), sem((3, 3)), sem((3, 3)), sem((3,)), sem((3,)), sem((3,)),
               sem((RING,)), sem((GROUPS,)), sem((2, GROUPS)), sem,
               sem((RING,)), sem((GROUPS,)), sem((3, GROUPS)), sem((2,)), sem, sem],
            compiler_params=pltpu.CompilerParams(has_side_effects=True, vmem_limit_bytes=63 * 1024 * 1024),
            name="moe_layer",
        )(idx_t, gate_t, tokens, w_gate[0], w_up[0], w_down[0])
        return out

    return jax.shard_map(device_step, mesh=mesh, in_specs=(row_spec, row_spec, row_spec, P('ep', 'fsdp', None), P('ep', 'fsdp', None), P('ep', None, 'fsdp')), out_specs=row_spec, check_vma=False)
```

```python
import functools

import jax
import jax.numpy as jnp
from jax import lax
from jax.experimental import pallas as pl
from jax.experimental.pallas import tpu as pltpu
from jax.sharding import PartitionSpec as P

F32 = jnp.float32
BF16 = jnp.bfloat16
MESH = pl.DeviceIdType.MESH
SIDE = 4
STRIDE = (16, 4, 1)
N_EXP = 64
GROUPS, PER = 8, 8
ROUTES = ((2, 1, 0), (1, 0, 2), (0, 2, 1))
OUT_ROUTES = ((0, 1, 2), (1, 2, 0), (2, 0, 1))
LEAD = 3
RING = 4


def hits(idx_t, eid):
    hit = jnp.zeros((eid.shape[0], idx_t.shape[1]), F32)
    for j in range(6):
        hit = jnp.where(idx_t[j:j + 1, :] == eid, 1.0, hit)
    return hit


def slot_keys(hit, earlier):
    before = jnp.dot(hit.astype(BF16), earlier, preferred_element_type=F32)
    return jnp.where(hit > 0.5, before, -1.0)


def offset(g, i):
    dz, b = i // 2, i % 2
    lean = 2 * b + lax.rem(g, 2)
    return dz, lax.rem(dz + lean, SIDE), lax.rem(lean + lax.div(g, 2) + SIDE - dz, SIDE)


def moved(d):
    return (d + SIDE - 1) // SIDE if isinstance(d, int) else lax.div(d + SIDE - 1, SIDE)


def if_moves(d, far, near=None):
    if isinstance(d, int):
        (far if d else near or (lambda: None))()
        return
    pl.when(d > 0)(far)
    if near is not None:
        pl.when(d == 0)(near)


def layer_kernel(cap, cuts, idx_ref, gate_ref, tok_ref, wg, wu, wd, out_ref, inbox, back,
                 wgu, wdn, toks_z, toks_y, toks_x, idx_all, keys, mixw, acc, stage, xbuf, outs, land,
                 ag_send, ag_recv, ix_send, ix_recv, own_sem, w_loc, w_send, w_recv,
                 d_send, d_keep, d_recv, d_relay, c_send, c_keep, c_recv, c_relay, x_sem, m_sem):
    tok, dim = acc.shape
    half, ffn = wg.shape
    rows = PER * cap
    far = rows // SIDE * (SIDE - 1)
    me = lax.axis_index('ep')
    core = lax.axis_index('fsdp')
    pos = (lax.div(me, 16), lax.rem(lax.div(me, 4), 4), lax.rem(me, 4))
    gathered = (toks_z, toks_y, toks_x)

    def shifted(a, k):
        return me + (lax.rem(pos[a] + k, SIDE) - pos[a]) * STRIDE[a]

    def ag_copies(a, k):
        dev = {'ep': shifted(a, k)}
        lo, hi = cuts[a], cuts[a + 1]
        yield pltpu.make_async_remote_copy(src_ref=idx_ref, dst_ref=idx_all.at[a, k - 1], send_sem=ix_send.at[a, k - 1],
                                           recv_sem=ix_recv.at[a, k - 1], device_id=dev, device_id_type=MESH)
        yield pltpu.make_async_remote_copy(src_ref=tok_ref.at[:, pl.ds(lo, hi - lo)], dst_ref=gathered[a].at[k],
                                           send_sem=ag_send.at[a, k - 1], recv_sem=ag_recv.at[a, k - 1],
                                           device_id=dev, device_id_type=MESH)

    barrier = pltpu.get_barrier_semaphore()
    for a in range(3):
        for k in range(1, SIDE):
            pl.semaphore_signal(barrier, inc=1, device_id={'ep': shifted(a, k)}, device_id_type=MESH)
    pl.semaphore_signal(barrier, inc=1, device_id={'fsdp': 1 - core}, device_id_type=MESH)

    at = pl.ds(pl.multiple_of(core * half, half), half)
    spots = ((wg, wgu.at[at, pl.ds(0, ffn)]), (wu, wgu.at[at, pl.ds(ffn, ffn)]), (wd, wdn.at[:, at]))
    w_copies = []
    for n, (src, dst) in enumerate(spots):
        w_copies.append(pltpu.make_async_copy(src, dst, w_loc.at[n]))
        w_copies.append(pltpu.make_async_remote_copy(src_ref=src, dst_ref=dst, send_sem=w_send.at[n], recv_sem=w_recv.at[n],
                                                     device_id={'fsdp': 1 - core}, device_id_type=MESH))

    own = [pltpu.make_async_copy(tok_ref.at[:, pl.ds(cuts[a], cuts[a + 1] - cuts[a])], gathered[a].at[0], own_sem.at[a]) for a in range(3)]
    for c in own:
        c.start()
    pl.semaphore_wait(barrier, 10)
    for k in (2, 1, 3):
        for a in range(3):
            for c in ag_copies(a, k):
                c.start()
    for c in w_copies:
        c.start()

    before = lax.broadcasted_iota(jnp.int32, (tok, tok), 0)
    after = lax.broadcasted_iota(jnp.int32, (tok, tok), 1)
    earlier = jnp.where(before < after, 1.0, 0.0).astype(BF16)
    slot = lax.broadcasted_iota(jnp.int32, (cap, tok), 0).astype(F32)

    def block(i, p):
        return pl.ds(i * cap, cap), pl.ds(cuts[p], cuts[p + 1] - cuts[p])

    def each(g, routes):
        for i in range(PER):
            ds = offset(g, i)
            for p in range(3):
                yield i, p, [ds[axis] for axis in routes[p]]

    def wait_rows(ref, n, sem):
        part = ref.at[pl.ds(0, n)]
        pltpu.make_async_copy(part, part, sem).wait()

    def plane_keys(a, k):
        q = lax.broadcasted_iota(jnp.int32, (16, 1), 0)
        _, b, c = OUT_ROUTES[a]
        eid = pos[a] * STRIDE[a] + ((pos[b] + (q >> 2)) & 3) * STRIDE[b] + ((pos[c] + (q & 3)) & 3) * STRIDE[c]
        ids = idx_ref[...] if k == 0 else idx_all[a, k - 1]
        keys[a, k] = slot_keys(hits(ids, eid), earlier)

    def back_of(d):
        return (SIDE - d) % SIDE if isinstance(d, int) else lax.rem(SIDE - d, SIDE)

    def pick(g):
        ring = lax.rem(g, RING)

        @pl.when(g >= RING)
        def _():
            wait_rows(stage.at[ring], far, d_send.at[ring])

        for i, p, d in each(g, OUT_ROUTES):
            lo, hi = cuts[p], cuts[p + 1]
            k = back_of(d[0])
            key = keys[p, k, pl.ds(back_of(d[1]) * 4 + back_of(d[2]), 1), :]
            sel = jnp.where(key == slot, 1.0, 0.0).astype(BF16)
            got = jnp.dot(sel, gathered[p][k], preferred_element_type=F32)
            stage[ring, i * cap:(i + 1) * cap, lo:hi] = got.astype(BF16)
        for i, p, d in each(g, OUT_ROUTES):
            src, dst = stage.at[ring, *block(i, p)], inbox.at[0, g, *block(i, p)]
            if_moves(d[1], lambda: pltpu.make_async_remote_copy(
                src_ref=src, dst_ref=dst, send_sem=d_send.at[ring], recv_sem=d_recv.at[0, g],
                device_id={'ep': shifted(OUT_ROUTES[p][1], back_of(d[1]))}, device_id_type=MESH).start(),
                lambda: pltpu.make_async_copy(src, dst, d_keep.at[g]).start())

    def forward(g):
        wait_rows(inbox.at[0, g], far, d_recv.at[0, g])
        wait_rows(inbox.at[0, g], rows - far, d_keep.at[g])
        for i, p, d in each(g, OUT_ROUTES):
            if_moves(d[2], lambda: pltpu.make_async_remote_copy(
                src_ref=inbox.at[0, g, *block(i, p)], dst_ref=inbox.at[1, g, *block(i, p)], send_sem=d_relay,
                recv_sem=d_recv.at[1, g], device_id={'ep': shifted(OUT_ROUTES[p][2], back_of(d[2]))}, device_id_type=MESH).start())

    def fetch(g):
        wait_rows(inbox.at[1, g], far, d_recv.at[1, g])
        for i, p, d in each(g, OUT_ROUTES):
            pltpu.make_async_copy(inbox.at[moved(d[2]), g, *block(i, p)], xbuf.at[block(i, p)], x_sem).start()

    def build_mix():
        idx_t, gate_t = idx_ref[...], gate_ref[...]
        eid = lax.broadcasted_iota(jnp.int32, (N_EXP, tok), 0)
        key = slot_keys(hits(idx_t, eid), earlier).astype(BF16)
        gate = jnp.zeros((N_EXP, tok), F32)
        for j in range(6):
            gate = jnp.where(idx_t[j:j + 1, :] == eid, gate_t[j:j + 1, :], gate)
        pieces = []
        left = gate
        for part in range(3):
            pieces.append(left.astype(BF16))
            left = left - pieces[-1].astype(F32)
        turn = functools.partial(lax.dot_general, dimension_numbers=(((0,), (0,)), ((), ())), preferred_element_type=F32)
        col = lax.broadcasted_iota(jnp.int32, (N_EXP, rows), 1)
        row = lax.broadcasted_iota(jnp.int32, (N_EXP, rows), 0)
        nth = jnp.zeros((N_EXP, rows), jnp.int32)
        for n in range(1, PER):
            nth = nth + jnp.where(col >= n * cap, 1, 0)
        want = (col - nth * cap)[0:1].astype(F32)
        dz = nth >> 1

        @pl.loop(0, GROUPS)
        def _(g):
            lean = (nth & 1) * 2 + lax.rem(g, 2)
            dy = (dz + lean) & 3
            dx = (lean + lax.div(g, 2) - dz) & 3
            exp = ((pos[0] - dz) & 3) * 16 + ((pos[1] - dy) & 3) * 4 + ((pos[2] - dx) & 3)
            spread = jnp.where(exp == row, 1.0, 0.0).astype(BF16)
            mine = turn(key, spread) == want
            span = pl.ds(pl.multiple_of(g * rows, 128), rows)
            for part in range(3):
                mixw[part * tok:(part + 1) * tok, span] = jnp.where(mine, turn(pieces[part], spread), 0.0).astype(BF16)

    def experts(g):
        ring = lax.rem(g, RING)
        pltpu.make_async_copy(xbuf, xbuf, x_sem).wait()

        @pl.when(g >= RING)
        def _():
            wait_rows(outs.at[ring], far, c_send.at[ring])

        both = jnp.dot(xbuf[...], wgu[...], preferred_element_type=F32)
        act_a, act_b = both[:, :ffn], both[:, ffn:]
        hidden = (act_a * jax.nn.sigmoid(act_a) * act_b).astype(BF16)
        outs[ring] = jnp.dot(hidden, wdn[...], preferred_element_type=F32).astype(BF16)
        for i, p, d in each(g, ROUTES):
            src = outs.at[ring, *block(i, p)]
            if_moves(d[0], lambda: hop(src, 0, g, i, p, d[0], c_send.at[ring]).start(),
                     lambda: pltpu.make_async_copy(src, back.at[0, g, *block(i, p)], c_keep.at[g]).start())

    def hop(src, leg, g, i, p, d, send):
        return pltpu.make_async_remote_copy(
            src_ref=src, dst_ref=back.at[leg, g, *block(i, p)], send_sem=send, recv_sem=c_recv.at[leg, g],
            device_id={'ep': shifted(ROUTES[p][leg], d)}, device_id_type=MESH)

    def second_hops(g):
        wait_rows(back.at[0, g], far, c_recv.at[0, g])
        wait_rows(back.at[0, g], rows - far, c_keep.at[g])
        for i, p, d in each(g, ROUTES):
            if_moves(d[1], lambda: hop(back.at[0, g, *block(i, p)], 1, g, i, p, d[1], c_relay.at[0]).start())

    def third_hops(g):
        wait_rows(back.at[1, g], far, c_recv.at[1, g])
        for i, p, d in each(g, ROUTES):
            if_moves(d[2], lambda: hop(back.at[moved(d[1]), g, *block(i, p)], 2, g, i, p, d[2], c_relay.at[1]).start())

    def mix(g):
        wait_rows(back.at[2, g], far, c_recv.at[2, g])
        for i, p, d in each(g, ROUTES):
            last = moved(d[2])
            leg = 2 * last + (1 - last) * moved(d[1])
            pltpu.make_async_copy(back.at[leg, g, *block(i, p)], land.at[block(i, p)], m_sem).start()
        pltpu.make_async_copy(land, land, m_sem).wait()
        w = mixw[:, pl.ds(pl.multiple_of(g * rows, 128), rows)]
        for n in range(0, dim, 512):
            parts = jnp.dot(w, land[:, n:n + 512], preferred_element_type=F32)
            acc[:, n:n + 512] += parts[:tok] + parts[tok:2 * tok] + parts[2 * tok:]

    for a in range(3):
        plane_keys(a, 0)
        own[a].wait()
        acc[:, cuts[a]:cuts[a + 1]] = gathered[a][0].astype(F32)
    for k in (1, 3, 2):
        for a in range(3):
            for c in ag_copies(a, k):
                c.wait_recv()
            plane_keys(a, k)
    for g in range(LEAD):
        pick(jnp.int32(g))
    build_mix()
    for a in range(3):
        for k in (2, 1, 3):
            for c in ag_copies(a, k):
                c.wait_send()

    def in_turn(r, lag, step):
        g = r - lag
        pl.when((g >= 0) & (g < GROUPS))(lambda: step(g))

    @pl.loop(0, GROUPS + 4)
    def _(r):
        @pl.when(r == 1)
        def _():
            for c in w_copies:
                c.wait()

        in_turn(r, 0, forward)
        in_turn(r, 1, fetch)
        pl.when(r + LEAD < GROUPS)(lambda: pick(r + LEAD))
        in_turn(r, 1, experts)
        in_turn(r, 2, second_hops)
        in_turn(r, 3, third_hops)
        in_turn(r, 4, mix)

    out_ref[...] = acc[...].astype(BF16)
    for ring in range(RING):
        wait_rows(stage.at[ring], far, d_send.at[ring])
        wait_rows(outs.at[ring], far, c_send.at[ring])
    for sem in (d_relay, c_relay.at[0], c_relay.at[1]):
        part = back.at[0, :, pl.ds(0, far)]
        pltpu.make_async_copy(part, part, sem).wait()


def solution(mesh):
    row_spec = P(('rep', 'ep', 'fsdp'), None)

    def device_step(tokens, expert_idx, gates, w_gate, w_up, w_down):
        tok, top_k = expert_idx.shape
        dim = tokens.shape[1]
        half, width = w_gate.shape[1:]
        cap = (2 * tok * top_k + N_EXP - 1) // N_EXP
        cuts = (0, 640, 1280, dim)
        rows = PER * cap
        idx_t = expert_idx.T
        gate_t = gates.T
        vmem = pl.BlockSpec(memory_space=pltpu.VMEM)
        hbm = pl.BlockSpec(memory_space=pl.ANY)
        sem = pltpu.SemaphoreType.DMA
        out, _, _ = pl.pallas_call(
            functools.partial(layer_kernel, cap, cuts),
            out_shape=(jax.ShapeDtypeStruct((tok, dim), BF16), jax.ShapeDtypeStruct((2, GROUPS, rows, dim), BF16),
                       jax.ShapeDtypeStruct((3, GROUPS, rows, dim), BF16)),
            in_specs=[vmem, vmem, hbm, hbm, hbm, hbm],
            out_specs=(vmem, hbm, hbm),
            scratch_shapes=[pltpu.VMEM((dim, 2 * width), BF16), pltpu.VMEM((width, dim), BF16)]
            + [pltpu.VMEM((SIDE, tok, cuts[a + 1] - cuts[a]), BF16) for a in range(3)]
            + [pltpu.VMEM((3, 3, top_k, tok), jnp.int32), pltpu.VMEM((3, SIDE, 16, tok), F32), pltpu.VMEM((3 * tok, N_EXP * cap), BF16),
               pltpu.VMEM((tok, dim), F32), pltpu.VMEM((RING, rows, dim), BF16), pltpu.VMEM((rows, dim), BF16),
               pltpu.VMEM((RING, rows, dim), BF16), pltpu.VMEM((rows, dim), BF16),
               sem((3, 3)), sem((3, 3)), sem((3, 3)), sem((3, 3)), sem((3,)), sem((3,)), sem((3,)), sem((3,)),
               sem((RING,)), sem((GROUPS,)), sem((2, GROUPS)), sem,
               sem((RING,)), sem((GROUPS,)), sem((3, GROUPS)), sem((2,)), sem, sem],
            compiler_params=pltpu.CompilerParams(collective_id=0, has_side_effects=True, vmem_limit_bytes=63 * 1024 * 1024),
            name="moe_layer",
        )(idx_t, gate_t, tokens, w_gate[0], w_up[0], w_down[0])
        return out

    return jax.shard_map(device_step, mesh=mesh, in_specs=(row_spec, row_spec, row_spec, P('ep', 'fsdp', None), P('ep', 'fsdp', None), P('ep', None, 'fsdp')), out_specs=row_spec, check_vma=False)
```

```python
import functools

import jax
import jax.numpy as jnp
from jax import lax
from jax.experimental import pallas as pl
from jax.experimental.pallas import tpu as pltpu
from jax.sharding import PartitionSpec as P

F32 = jnp.float32
BF16 = jnp.bfloat16
MESH = pl.DeviceIdType.MESH
SIDE = 4
STRIDE = (16, 4, 1)
N_EXP = 64
GROUPS, PER = 8, 8
ROUTES = ((2, 1, 0), (1, 0, 2), (0, 2, 1))
OUT_ROUTES = ((0, 1, 2), (1, 2, 0), (2, 0, 1))
LEAD = 3
RING = 4


def hits(idx_t, eid):
    hit = jnp.zeros((eid.shape[0], idx_t.shape[1]), F32)
    for j in range(6):
        hit = jnp.where(idx_t[j:j + 1, :] == eid, 1.0, hit)
    return hit


def slot_keys(hit, earlier):
    before = jnp.dot(hit.astype(BF16), earlier, preferred_element_type=F32)
    return jnp.where(hit > 0.5, before, -1.0)


def offset(g, i):
    dz, b = i // 2, i % 2
    fixed = isinstance(g, int)
    low, high = (g % 2, g // 2) if fixed else (lax.rem(g, 2), lax.div(g, 2))
    lean = 2 * b + low
    dy, dx = dz + lean, lean + high + SIDE - dz
    return (dz, dy % SIDE, dx % SIDE) if fixed else (dz, lax.rem(dy, SIDE), lax.rem(dx, SIDE))


def moved(d):
    return (d + SIDE - 1) // SIDE if isinstance(d, int) else lax.div(d + SIDE - 1, SIDE)


def if_moves(d, far, near=None):
    if isinstance(d, int):
        (far if d else near or (lambda: None))()
        return
    pl.when(d > 0)(far)
    if near is not None:
        pl.when(d == 0)(near)


def layer_kernel(cap, cuts, idx_ref, gate_ref, tok_ref, wg, wu, wd, out_ref, inbox, back,
                 wgu, wdn, toks_z, toks_y, toks_x, idx_all, keys, mixw, acc, stage, xbuf, outs, land,
                 ag_send, ag_recv, ix_send, ix_recv, own_sem, w_loc, w_send, w_recv,
                 d_send, d_keep, d_recv, d_relay, c_send, c_keep, c_recv, c_relay, x_sem, m_sem):
    tok, dim = acc.shape
    half, ffn = wg.shape
    rows = PER * cap
    far = rows // SIDE * (SIDE - 1)
    me = lax.axis_index('ep')
    core = lax.axis_index('fsdp')
    pos = (lax.div(me, 16), lax.rem(lax.div(me, 4), 4), lax.rem(me, 4))
    gathered = (toks_z, toks_y, toks_x)

    def shifted(a, k):
        return me + (lax.rem(pos[a] + k, SIDE) - pos[a]) * STRIDE[a]

    def ag_copies(a, k):
        dev = {'ep': shifted(a, k)}
        lo, hi = cuts[a], cuts[a + 1]
        yield pltpu.make_async_remote_copy(src_ref=idx_ref, dst_ref=idx_all.at[a, k - 1], send_sem=ix_send.at[a, k - 1],
                                           recv_sem=ix_recv.at[a, k - 1], device_id=dev, device_id_type=MESH)
        yield pltpu.make_async_remote_copy(src_ref=tok_ref.at[:, pl.ds(lo, hi - lo)], dst_ref=gathered[a].at[k],
                                           send_sem=ag_send.at[a, k - 1], recv_sem=ag_recv.at[a, k - 1],
                                           device_id=dev, device_id_type=MESH)

    barrier = pltpu.get_barrier_semaphore()
    for a in range(3):
        for k in range(1, SIDE):
            pl.semaphore_signal(barrier, inc=1, device_id={'ep': shifted(a, k)}, device_id_type=MESH)
    pl.semaphore_signal(barrier, inc=1, device_id={'fsdp': 1 - core}, device_id_type=MESH)

    at = pl.ds(pl.multiple_of(core * half, half), half)
    spots = ((wg, wgu.at[at, pl.ds(0, ffn)]), (wu, wgu.at[at, pl.ds(ffn, ffn)]), (wd, wdn.at[:, at]))
    w_copies = []
    for n, (src, dst) in enumerate(spots):
        w_copies.append(pltpu.make_async_copy(src, dst, w_loc.at[n]))
        w_copies.append(pltpu.make_async_remote_copy(src_ref=src, dst_ref=dst, send_sem=w_send.at[n], recv_sem=w_recv.at[n],
                                                     device_id={'fsdp': 1 - core}, device_id_type=MESH))

    own = [pltpu.make_async_copy(tok_ref.at[:, pl.ds(cuts[a], cuts[a + 1] - cuts[a])], gathered[a].at[0], own_sem.at[a]) for a in range(3)]
    for c in own:
        c.start()
    pl.semaphore_wait(barrier, 10)
    for k in (1, 3, 2):
        for a in range(3):
            for c in ag_copies(a, k):
                c.start()
    for c in w_copies:
        c.start()

    before = lax.broadcasted_iota(jnp.int32, (tok, tok), 0)
    after = lax.broadcasted_iota(jnp.int32, (tok, tok), 1)
    earlier = jnp.where(before < after, 1.0, 0.0).astype(BF16)
    slot = lax.broadcasted_iota(jnp.int32, (cap, tok), 0).astype(F32)

    def block(i, p):
        return pl.ds(i * cap, cap), pl.ds(cuts[p], cuts[p + 1] - cuts[p])

    def each(g, routes):
        for i in range(PER):
            ds = offset(g, i)
            for p in range(3):
                yield i, p, [ds[axis] for axis in routes[p]]

    def wait_rows(ref, n, sem):
        part = ref.at[pl.ds(0, n)]
        pltpu.make_async_copy(part, part, sem).wait()

    def plane_keys(a, k):
        q = lax.broadcasted_iota(jnp.int32, (16, 1), 0)
        _, b, c = OUT_ROUTES[a]
        eid = pos[a] * STRIDE[a] + ((pos[b] + (q >> 2)) & 3) * STRIDE[b] + ((pos[c] + (q & 3)) & 3) * STRIDE[c]
        ids = idx_ref[...] if k == 0 else idx_all[a, k - 1]
        keys[a, k] = slot_keys(hits(ids, eid), earlier)

    def back_of(d):
        return (SIDE - d) % SIDE if isinstance(d, int) else lax.rem(SIDE - d, SIDE)

    def pick(g):
        ring = lax.rem(g, RING)

        @pl.when(g >= RING)
        def _():
            wait_rows(stage.at[ring], far, d_send.at[ring])

        pick_blocks(g, ring, list(each(g, OUT_ROUTES)))

    def pick_blocks(g, ring, blocks):
        for i, p, d in blocks:
            lo, hi = cuts[p], cuts[p + 1]
            k = back_of(d[0])
            key = keys[p, k, pl.ds(back_of(d[1]) * 4 + back_of(d[2]), 1), :]
            sel = jnp.where(key == slot, 1.0, 0.0).astype(BF16)
            got = jnp.dot(sel, gathered[p][k], preferred_element_type=F32)
            stage[ring, i * cap:(i + 1) * cap, lo:hi] = got.astype(BF16)
        for i, p, d in blocks:
            src, dst = stage.at[ring, *block(i, p)], inbox.at[0, g, *block(i, p)]
            if_moves(d[1], lambda: pltpu.make_async_remote_copy(
                src_ref=src, dst_ref=dst, send_sem=d_send.at[ring], recv_sem=d_recv.at[0, g],
                device_id={'ep': shifted(OUT_ROUTES[p][1], back_of(d[1]))}, device_id_type=MESH).start(),
                lambda: pltpu.make_async_copy(src, dst, d_keep.at[g]).start())

    def early_picks(k):
        for g in range(LEAD):
            pick_blocks(g, g, [(i, p, d) for i, p, d in each(g, OUT_ROUTES) if back_of(d[0]) == k])

    def forward(g):
        wait_rows(inbox.at[0, g], far, d_recv.at[0, g])
        wait_rows(inbox.at[0, g], rows - far, d_keep.at[g])
        for i, p, d in each(g, OUT_ROUTES):
            if_moves(d[2], lambda: pltpu.make_async_remote_copy(
                src_ref=inbox.at[0, g, *block(i, p)], dst_ref=inbox.at[1, g, *block(i, p)], send_sem=d_relay,
                recv_sem=d_recv.at[1, g], device_id={'ep': shifted(OUT_ROUTES[p][2], back_of(d[2]))}, device_id_type=MESH).start())

    def fetch(g):
        wait_rows(inbox.at[1, g], far, d_recv.at[1, g])
        for i, p, d in each(g, OUT_ROUTES):
            pltpu.make_async_copy(inbox.at[moved(d[2]), g, *block(i, p)], xbuf.at[block(i, p)], x_sem).start()

    def build_mix():
        idx_t, gate_t = idx_ref[...], gate_ref[...]
        eid = lax.broadcasted_iota(jnp.int32, (N_EXP, tok), 0)
        key = slot_keys(hits(idx_t, eid), earlier).astype(BF16)
        gate = jnp.zeros((N_EXP, tok), F32)
        for j in range(6):
            gate = jnp.where(idx_t[j:j + 1, :] == eid, gate_t[j:j + 1, :], gate)
        pieces = []
        left = gate
        for part in range(3):
            pieces.append(left.astype(BF16))
            left = left - pieces[-1].astype(F32)
        turn = functools.partial(lax.dot_general, dimension_numbers=(((0,), (0,)), ((), ())), preferred_element_type=F32)
        col = lax.broadcasted_iota(jnp.int32, (N_EXP, rows), 1)
        row = lax.broadcasted_iota(jnp.int32, (N_EXP, rows), 0)
        nth = jnp.zeros((N_EXP, rows), jnp.int32)
        for n in range(1, PER):
            nth = nth + jnp.where(col >= n * cap, 1, 0)
        want = (col - nth * cap)[0:1].astype(F32)
        dz = nth >> 1

        @pl.loop(0, GROUPS)
        def _(g):
            lean = (nth & 1) * 2 + lax.rem(g, 2)
            dy = (dz + lean) & 3
            dx = (lean + lax.div(g, 2) - dz) & 3
            exp = ((pos[0] - dz) & 3) * 16 + ((pos[1] - dy) & 3) * 4 + ((pos[2] - dx) & 3)
            spread = jnp.where(exp == row, 1.0, 0.0).astype(BF16)
            mine = turn(key, spread) == want
            span = pl.ds(pl.multiple_of(g * rows, 128), rows)
            for part in range(3):
                mixw[part * tok:(part + 1) * tok, span] = jnp.where(mine, turn(pieces[part], spread), 0.0).astype(BF16)

    def experts(g):
        ring = lax.rem(g, RING)
        pltpu.make_async_copy(xbuf, xbuf, x_sem).wait()

        @pl.when(g >= RING)
        def _():
            wait_rows(outs.at[ring], far, c_send.at[ring])

        both = jnp.dot(xbuf[...], wgu[...], preferred_element_type=F32)
        act_a, act_b = both[:, :ffn], both[:, ffn:]
        hidden = (act_a * jax.nn.sigmoid(act_a) * act_b).astype(BF16)
        outs[ring] = jnp.dot(hidden, wdn[...], preferred_element_type=F32).astype(BF16)
        for i, p, d in each(g, ROUTES):
            src = outs.at[ring, *block(i, p)]
            if_moves(d[0], lambda: hop(src, 0, g, i, p, d[0], c_send.at[ring]).start(),
                     lambda: pltpu.make_async_copy(src, back.at[0, g, *block(i, p)], c_keep.at[g]).start())

    def hop(src, leg, g, i, p, d, send):
        return pltpu.make_async_remote_copy(
            src_ref=src, dst_ref=back.at[leg, g, *block(i, p)], send_sem=send, recv_sem=c_recv.at[leg, g],
            device_id={'ep': shifted(ROUTES[p][leg], d)}, device_id_type=MESH)

    def second_hops(g):
        wait_rows(back.at[0, g], far, c_recv.at[0, g])
        wait_rows(back.at[0, g], rows - far, c_keep.at[g])
        for i, p, d in each(g, ROUTES):
            if_moves(d[1], lambda: hop(back.at[0, g, *block(i, p)], 1, g, i, p, d[1], c_relay.at[0]).start())

    def third_hops(g):
        wait_rows(back.at[1, g], far, c_recv.at[1, g])
        for i, p, d in each(g, ROUTES):
            if_moves(d[2], lambda: hop(back.at[moved(d[1]), g, *block(i, p)], 2, g, i, p, d[2], c_relay.at[1]).start())

    def mix(g):
        wait_rows(back.at[2, g], far, c_recv.at[2, g])
        for i, p, d in each(g, ROUTES):
            last = moved(d[2])
            leg = 2 * last + (1 - last) * moved(d[1])
            pltpu.make_async_copy(back.at[leg, g, *block(i, p)], land.at[block(i, p)], m_sem).start()
        pltpu.make_async_copy(land, land, m_sem).wait()
        w = mixw[:, pl.ds(pl.multiple_of(g * rows, 128), rows)]
        for n in range(0, dim, 512):
            parts = jnp.dot(w, land[:, n:n + 512], preferred_element_type=F32)
            acc[:, n:n + 512] += parts[:tok] + parts[tok:2 * tok] + parts[2 * tok:]

    for a in range(3):
        plane_keys(a, 0)
        own[a].wait()
        acc[:, cuts[a]:cuts[a + 1]] = gathered[a][0].astype(F32)
    early_picks(0)
    for k in (1, 3, 2):
        for a in range(3):
            for c in ag_copies(a, k):
                c.wait_recv()
            plane_keys(a, k)
        early_picks(k)
    build_mix()
    for a in range(3):
        for k in (2, 1, 3):
            for c in ag_copies(a, k):
                c.wait_send()

    def in_turn(r, lag, step):
        g = r - lag
        pl.when((g >= 0) & (g < GROUPS))(lambda: step(g))

    @pl.loop(0, GROUPS + 4)
    def _(r):
        @pl.when(r == 1)
        def _():
            for c in w_copies:
                c.wait()

        in_turn(r, 0, forward)
        in_turn(r, 1, fetch)
        pl.when(r + LEAD < GROUPS)(lambda: pick(r + LEAD))
        in_turn(r, 1, experts)
        in_turn(r, 2, second_hops)
        in_turn(r, 3, third_hops)
        in_turn(r, 4, mix)

    out_ref[...] = acc[...].astype(BF16)
    for ring in range(RING):
        wait_rows(stage.at[ring], far, d_send.at[ring])
        wait_rows(outs.at[ring], far, c_send.at[ring])
    for sem in (d_relay, c_relay.at[0], c_relay.at[1]):
        part = back.at[0, :, pl.ds(0, far)]
        pltpu.make_async_copy(part, part, sem).wait()


def solution(mesh):
    row_spec = P(('rep', 'ep', 'fsdp'), None)

    def device_step(tokens, expert_idx, gates, w_gate, w_up, w_down):
        tok, top_k = expert_idx.shape
        dim = tokens.shape[1]
        half, width = w_gate.shape[1:]
        cap = (2 * tok * top_k + N_EXP - 1) // N_EXP
        cuts = (0, 640, 1280, dim)
        rows = PER * cap
        idx_t = expert_idx.T
        gate_t = gates.T
        vmem = pl.BlockSpec(memory_space=pltpu.VMEM)
        hbm = pl.BlockSpec(memory_space=pl.ANY)
        sem = pltpu.SemaphoreType.DMA
        out, _, _ = pl.pallas_call(
            functools.partial(layer_kernel, cap, cuts),
            out_shape=(jax.ShapeDtypeStruct((tok, dim), BF16), jax.ShapeDtypeStruct((2, GROUPS, rows, dim), BF16),
                       jax.ShapeDtypeStruct((3, GROUPS, rows, dim), BF16)),
            in_specs=[vmem, vmem, hbm, hbm, hbm, hbm],
            out_specs=(vmem, hbm, hbm),
            scratch_shapes=[pltpu.VMEM((dim, 2 * width), BF16), pltpu.VMEM((width, dim), BF16)]
            + [pltpu.VMEM((SIDE, tok, cuts[a + 1] - cuts[a]), BF16) for a in range(3)]
            + [pltpu.VMEM((3, 3, top_k, tok), jnp.int32), pltpu.VMEM((3, SIDE, 16, tok), F32), pltpu.VMEM((3 * tok, N_EXP * cap), BF16),
               pltpu.VMEM((tok, dim), F32), pltpu.VMEM((RING, rows, dim), BF16), pltpu.VMEM((rows, dim), BF16),
               pltpu.VMEM((RING, rows, dim), BF16), pltpu.VMEM((rows, dim), BF16),
               sem((3, 3)), sem((3, 3)), sem((3, 3)), sem((3, 3)), sem((3,)), sem((3,)), sem((3,)), sem((3,)),
               sem((RING,)), sem((GROUPS,)), sem((2, GROUPS)), sem,
               sem((RING,)), sem((GROUPS,)), sem((3, GROUPS)), sem((2,)), sem, sem],
            compiler_params=pltpu.CompilerParams(collective_id=0, has_side_effects=True, vmem_limit_bytes=63 * 1024 * 1024),
            name="moe_layer",
        )(idx_t, gate_t, tokens, w_gate[0], w_up[0], w_down[0])
        return out

    return jax.shard_map(device_step, mesh=mesh, in_specs=(row_spec, row_spec, row_spec, P('ep', 'fsdp', None), P('ep', 'fsdp', None), P('ep', None, 'fsdp')), out_specs=row_spec, check_vma=False)
```

```python
import functools

import jax
import jax.numpy as jnp
from jax import lax
from jax.experimental import pallas as pl
from jax.experimental.pallas import tpu as pltpu
from jax.sharding import PartitionSpec as P

F32 = jnp.float32
BF16 = jnp.bfloat16
MESH = pl.DeviceIdType.MESH
SIDE = 4
STRIDE = (16, 4, 1)
N_EXP = 64
GROUPS, PER = 8, 8
ROUTES = ((2, 1, 0), (1, 0, 2), (0, 2, 1))
OUT_ROUTES = ((0, 1, 2), (1, 2, 0), (2, 0, 1))
LEAD = 3
RING = 4


def hits(idx_t, eid):
    hit = jnp.zeros((eid.shape[0], idx_t.shape[1]), F32)
    for j in range(6):
        hit = jnp.where(idx_t[j:j + 1, :] == eid, 1.0, hit)
    return hit


def slot_keys(hit, earlier):
    before = jnp.dot(hit.astype(BF16), earlier, preferred_element_type=F32)
    return jnp.where(hit > 0.5, before, -1.0)


def offset(g, i):
    dz, b = i // 2, i % 2
    fixed = isinstance(g, int)
    low, high = (g % 2, g // 2) if fixed else (lax.rem(g, 2), lax.div(g, 2))
    lean = 2 * b + low
    dy, dx = dz + lean, lean + high + SIDE - dz
    return (dz, dy % SIDE, dx % SIDE) if fixed else (dz, lax.rem(dy, SIDE), lax.rem(dx, SIDE))


def moved(d):
    return (d + SIDE - 1) // SIDE if isinstance(d, int) else lax.div(d + SIDE - 1, SIDE)


def if_moves(d, far, near=None):
    if isinstance(d, int):
        (far if d else near or (lambda: None))()
        return
    pl.when(d > 0)(far)
    if near is not None:
        pl.when(d == 0)(near)


def layer_kernel(cap, cuts, idx_hbm, gate_hbm, tok_ref, wg, wu, wd, out_ref, inbox, back,
                 wgu, wdn, toks_z, toks_y, toks_x, idx_all, idx_ref, gate_ref, keys, mixw, acc, stage, xbuf, outs, land,
                 ag_send, ag_recv, ix_send, ix_recv, on_send, on_recv, own_sem, w_loc, w_send, w_recv,
                 d_send, d_keep, d_recv, d_relay, c_send, c_keep, c_recv, c_relay, x_sem, m_sem):
    tok, dim = acc.shape
    half, ffn = wg.shape
    rows = PER * cap
    far = rows // SIDE * (SIDE - 1)
    me = lax.axis_index('ep')
    core = lax.axis_index('fsdp')
    pos = (lax.div(me, 16), lax.rem(lax.div(me, 4), 4), lax.rem(me, 4))
    gathered = (toks_z, toks_y, toks_x)

    def shifted(a, k):
        return me + (lax.rem(pos[a] + k, SIDE) - pos[a]) * STRIDE[a]

    def ag_copies(a, k):
        dev = {'ep': shifted(a, k)}
        lo, hi = cuts[a], cuts[a + 1]
        yield pltpu.make_async_remote_copy(src_ref=idx_hbm, dst_ref=idx_all.at[a, k - 1], send_sem=ix_send.at[a, k - 1],
                                           recv_sem=ix_recv.at[a, k - 1], device_id=dev, device_id_type=MESH)
        if k != 2:
            yield pltpu.make_async_remote_copy(src_ref=tok_ref.at[:, pl.ds(lo, hi - lo)], dst_ref=gathered[a].at[k],
                                               send_sem=ag_send.at[a, k - 1], recv_sem=ag_recv.at[a, k - 1],
                                               device_id=dev, device_id_type=MESH)

    def pass_on(a, k):
        part = pl.ds(0 if k == 1 else tok // 2, tok // 2)
        return pltpu.make_async_remote_copy(src_ref=gathered[a].at[k, part], dst_ref=gathered[a].at[2, part],
                                            send_sem=on_send.at[a, k // 2], recv_sem=on_recv.at[a, k // 2],
                                            device_id={'ep': shifted(a, k)}, device_id_type=MESH)

    barrier = pltpu.get_barrier_semaphore()
    for a in range(3):
        for k in range(1, SIDE):
            pl.semaphore_signal(barrier, inc=1, device_id={'ep': shifted(a, k)}, device_id_type=MESH)
    pl.semaphore_signal(barrier, inc=1, device_id={'fsdp': 1 - core}, device_id_type=MESH)

    at = pl.ds(pl.multiple_of(core * half, half), half)
    spots = ((wg, wgu.at[at, pl.ds(0, ffn)]), (wu, wgu.at[at, pl.ds(ffn, ffn)]), (wd, wdn.at[:, at]))
    w_copies = []
    for n, (src, dst) in enumerate(spots):
        w_copies.append(pltpu.make_async_copy(src, dst, w_loc.at[n]))
        w_copies.append(pltpu.make_async_remote_copy(src_ref=src, dst_ref=dst, send_sem=w_send.at[n], recv_sem=w_recv.at[n],
                                                     device_id={'fsdp': 1 - core}, device_id_type=MESH))

    own = [pltpu.make_async_copy(tok_ref.at[:, pl.ds(cuts[a], cuts[a + 1] - cuts[a])], gathered[a].at[0], own_sem.at[a]) for a in range(3)]
    own += [pltpu.make_async_copy(idx_hbm, idx_ref, own_sem.at[3]), pltpu.make_async_copy(gate_hbm, gate_ref, own_sem.at[4])]
    for c in own[::-1]:
        c.start()
    pl.semaphore_wait(barrier, 10)
    for k in (1, 3, 2):
        for a in range(3):
            for c in ag_copies(a, k):
                c.start()
    for c in w_copies:
        c.start()

    before = lax.broadcasted_iota(jnp.int32, (tok, tok), 0)
    after = lax.broadcasted_iota(jnp.int32, (tok, tok), 1)
    earlier = jnp.where(before < after, 1.0, 0.0).astype(BF16)
    slot = lax.broadcasted_iota(jnp.int32, (cap, tok), 0).astype(F32)

    def block(i, p):
        return pl.ds(i * cap, cap), pl.ds(cuts[p], cuts[p + 1] - cuts[p])

    def each(g, routes):
        for i in range(PER):
            ds = offset(g, i)
            for p in range(3):
                yield i, p, [ds[axis] for axis in routes[p]]

    def wait_rows(ref, n, sem):
        part = ref.at[pl.ds(0, n)]
        pltpu.make_async_copy(part, part, sem).wait()

    def plane_keys(a, k):
        q = lax.broadcasted_iota(jnp.int32, (16, 1), 0)
        _, b, c = OUT_ROUTES[a]
        eid = pos[a] * STRIDE[a] + ((pos[b] + (q >> 2)) & 3) * STRIDE[b] + ((pos[c] + (q & 3)) & 3) * STRIDE[c]
        ids = idx_ref[...] if k == 0 else idx_all[a, k - 1]
        keys[a, k] = slot_keys(hits(ids, eid), earlier)

    def back_of(d):
        return (SIDE - d) % SIDE if isinstance(d, int) else lax.rem(SIDE - d, SIDE)

    def pick(g):
        ring = lax.rem(g, RING)

        @pl.when(g >= RING)
        def _():
            wait_rows(stage.at[ring], far, d_send.at[ring])

        pick_blocks(g, ring, list(each(g, OUT_ROUTES)))

    def pick_blocks(g, ring, blocks):
        for i, p, d in blocks:
            lo, hi = cuts[p], cuts[p + 1]
            k = back_of(d[0])
            key = keys[p, k, pl.ds(back_of(d[1]) * 4 + back_of(d[2]), 1), :]
            sel = jnp.where(key == slot, 1.0, 0.0).astype(BF16)
            got = jnp.dot(sel, gathered[p][k], preferred_element_type=F32)
            stage[ring, i * cap:(i + 1) * cap, lo:hi] = got.astype(BF16)
        for i, p, d in blocks:
            src, dst = stage.at[ring, *block(i, p)], inbox.at[0, g, *block(i, p)]
            if_moves(d[1], lambda: pltpu.make_async_remote_copy(
                src_ref=src, dst_ref=dst, send_sem=d_send.at[ring], recv_sem=d_recv.at[0, g],
                device_id={'ep': shifted(OUT_ROUTES[p][1], back_of(d[1]))}, device_id_type=MESH).start(),
                lambda: pltpu.make_async_copy(src, dst, d_keep.at[g]).start())

    def early_picks(k):
        for g in range(LEAD):
            pick_blocks(g, g, [(i, p, d) for i, p, d in each(g, OUT_ROUTES) if back_of(d[0]) == k])

    def forward(g):
        wait_rows(inbox.at[0, g], far, d_recv.at[0, g])
        wait_rows(inbox.at[0, g], rows - far, d_keep.at[g])
        for i, p, d in each(g, OUT_ROUTES):
            if_moves(d[2], lambda: pltpu.make_async_remote_copy(
                src_ref=inbox.at[0, g, *block(i, p)], dst_ref=inbox.at[1, g, *block(i, p)], send_sem=d_relay,
                recv_sem=d_recv.at[1, g], device_id={'ep': shifted(OUT_ROUTES[p][2], back_of(d[2]))}, device_id_type=MESH).start())

    def fetch(g):
        wait_rows(inbox.at[1, g], far, d_recv.at[1, g])
        for i, p, d in each(g, OUT_ROUTES):
            pltpu.make_async_copy(inbox.at[moved(d[2]), g, *block(i, p)], xbuf.at[block(i, p)], x_sem).start()

    def build_mix():
        idx_t, gate_t = idx_ref[...], gate_ref[...]
        eid = lax.broadcasted_iota(jnp.int32, (N_EXP, tok), 0)
        key = slot_keys(hits(idx_t, eid), earlier).astype(BF16)
        gate = jnp.zeros((N_EXP, tok), F32)
        for j in range(6):
            gate = jnp.where(idx_t[j:j + 1, :] == eid, gate_t[j:j + 1, :], gate)
        pieces = []
        left = gate
        for part in range(3):
            pieces.append(left.astype(BF16))
            left = left - pieces[-1].astype(F32)
        turn = functools.partial(lax.dot_general, dimension_numbers=(((0,), (0,)), ((), ())), preferred_element_type=F32)
        col = lax.broadcasted_iota(jnp.int32, (N_EXP, rows), 1)
        row = lax.broadcasted_iota(jnp.int32, (N_EXP, rows), 0)
        nth = jnp.zeros((N_EXP, rows), jnp.int32)
        for n in range(1, PER):
            nth = nth + jnp.where(col >= n * cap, 1, 0)
        want = (col - nth * cap)[0:1].astype(F32)
        dz = nth >> 1

        @pl.loop(0, GROUPS)
        def _(g):
            lean = (nth & 1) * 2 + lax.rem(g, 2)
            dy = (dz + lean) & 3
            dx = (lean + lax.div(g, 2) - dz) & 3
            exp = ((pos[0] - dz) & 3) * 16 + ((pos[1] - dy) & 3) * 4 + ((pos[2] - dx) & 3)
            spread = jnp.where(exp == row, 1.0, 0.0).astype(BF16)
            mine = turn(key, spread) == want
            span = pl.ds(pl.multiple_of(g * rows, 128), rows)
            for part in range(3):
                mixw[part * tok:(part + 1) * tok, span] = jnp.where(mine, turn(pieces[part], spread), 0.0).astype(BF16)

    def experts(g):
        ring = lax.rem(g, RING)
        pltpu.make_async_copy(xbuf, xbuf, x_sem).wait()

        @pl.when(g >= RING)
        def _():
            wait_rows(outs.at[ring], far, c_send.at[ring])

        both = jnp.dot(xbuf[...], wgu[...], preferred_element_type=F32)
        act_a, act_b = both[:, :ffn], both[:, ffn:]
        hidden = (act_a * jax.nn.sigmoid(act_a) * act_b).astype(BF16)
        outs[ring] = jnp.dot(hidden, wdn[...], preferred_element_type=F32).astype(BF16)
        for i, p, d in each(g, ROUTES):
            src = outs.at[ring, *block(i, p)]
            if_moves(d[0], lambda: hop(src, 0, g, i, p, d[0], c_send.at[ring]).start(),
                     lambda: pltpu.make_async_copy(src, back.at[0, g, *block(i, p)], c_keep.at[g]).start())

    def hop(src, leg, g, i, p, d, send):
        return pltpu.make_async_remote_copy(
            src_ref=src, dst_ref=back.at[leg, g, *block(i, p)], send_sem=send, recv_sem=c_recv.at[leg, g],
            device_id={'ep': shifted(ROUTES[p][leg], d)}, device_id_type=MESH)

    def second_hops(g):
        wait_rows(back.at[0, g], far, c_recv.at[0, g])
        wait_rows(back.at[0, g], rows - far, c_keep.at[g])
        for i, p, d in each(g, ROUTES):
            if_moves(d[1], lambda: hop(back.at[0, g, *block(i, p)], 1, g, i, p, d[1], c_relay.at[0]).start())

    def third_hops(g):
        wait_rows(back.at[1, g], far, c_recv.at[1, g])
        for i, p, d in each(g, ROUTES):
            if_moves(d[2], lambda: hop(back.at[moved(d[1]), g, *block(i, p)], 2, g, i, p, d[2], c_relay.at[1]).start())

    def mix(g):
        wait_rows(back.at[2, g], far, c_recv.at[2, g])
        for i, p, d in each(g, ROUTES):
            last = moved(d[2])
            leg = 2 * last + (1 - last) * moved(d[1])
            pltpu.make_async_copy(back.at[leg, g, *block(i, p)], land.at[block(i, p)], m_sem).start()
        pltpu.make_async_copy(land, land, m_sem).wait()
        w = mixw[:, pl.ds(pl.multiple_of(g * rows, 128), rows)]
        for n in range(0, dim, 512):
            parts = jnp.dot(w, land[:, n:n + 512], preferred_element_type=F32)
            acc[:, n:n + 512] += parts[:tok] + parts[tok:2 * tok] + parts[2 * tok:]

    own[3].wait()
    own[4].wait()
    for a in range(3):
        plane_keys(a, 0)
        own[a].wait()
        acc[:, cuts[a]:cuts[a + 1]] = gathered[a][0].astype(F32)
    early_picks(0)
    for k in (1, 3):
        for a in range(3):
            for c in ag_copies(a, k):
                c.wait_recv()
            pass_on(a, k).start()
    for k in (1, 3, 2):
        for a in range(3):
            if k == 2:
                for c in ag_copies(a, k):
                    c.wait_recv()
                pass_on(a, 1).wait_recv()
                pass_on(a, 3).wait_recv()
            plane_keys(a, k)
        early_picks(k)
    build_mix()
    for a in range(3):
        for k in (2, 1, 3):
            for c in ag_copies(a, k):
                c.wait_send()
        pass_on(a, 1).wait_send()
        pass_on(a, 3).wait_send()

    def in_turn(r, lag, step):
        g = r - lag
        pl.when((g >= 0) & (g < GROUPS))(lambda: step(g))

    @pl.loop(0, GROUPS + 4)
    def _(r):
        @pl.when(r == 1)
        def _():
            for c in w_copies:
                c.wait()

        in_turn(r, 0, forward)
        in_turn(r, 1, fetch)
        pl.when(r + LEAD < GROUPS)(lambda: pick(r + LEAD))
        in_turn(r, 1, experts)
        in_turn(r, 2, second_hops)
        in_turn(r, 3, third_hops)
        in_turn(r, 4, mix)

    out_ref[...] = acc[...].astype(BF16)
    for ring in range(RING):
        wait_rows(stage.at[ring], far, d_send.at[ring])
        wait_rows(outs.at[ring], far, c_send.at[ring])
    for sem in (d_relay, c_relay.at[0], c_relay.at[1]):
        part = back.at[0, :, pl.ds(0, far)]
        pltpu.make_async_copy(part, part, sem).wait()


def solution(mesh):
    row_spec = P(('rep', 'ep', 'fsdp'), None)

    def device_step(tokens, expert_idx, gates, w_gate, w_up, w_down):
        tok, top_k = expert_idx.shape
        dim = tokens.shape[1]
        half, width = w_gate.shape[1:]
        cap = (2 * tok * top_k + N_EXP - 1) // N_EXP
        cuts = (0, 640, 1280, dim)
        rows = PER * cap
        idx_t = expert_idx.T
        gate_t = gates.T
        vmem = pl.BlockSpec(memory_space=pltpu.VMEM)
        hbm = pl.BlockSpec(memory_space=pl.ANY)
        sem = pltpu.SemaphoreType.DMA
        out, _, _ = pl.pallas_call(
            functools.partial(layer_kernel, cap, cuts),
            out_shape=(jax.ShapeDtypeStruct((tok, dim), BF16), jax.ShapeDtypeStruct((2, GROUPS, rows, dim), BF16),
                       jax.ShapeDtypeStruct((3, GROUPS, rows, dim), BF16)),
            in_specs=[hbm] * 6,
            out_specs=(vmem, hbm, hbm),
            scratch_shapes=[pltpu.VMEM((dim, 2 * width), BF16), pltpu.VMEM((width, dim), BF16)]
            + [pltpu.VMEM((SIDE, tok, cuts[a + 1] - cuts[a]), BF16) for a in range(3)]
            + [pltpu.VMEM((3, 3, top_k, tok), jnp.int32), pltpu.VMEM((top_k, tok), jnp.int32), pltpu.VMEM((top_k, tok), F32), pltpu.VMEM((3, SIDE, 16, tok), F32), pltpu.VMEM((3 * tok, N_EXP * cap), BF16),
               pltpu.VMEM((tok, dim), F32), pltpu.VMEM((RING, rows, dim), BF16), pltpu.VMEM((rows, dim), BF16),
               pltpu.VMEM((RING, rows, dim), BF16), pltpu.VMEM((rows, dim), BF16),
               sem((3, 3)), sem((3, 3)), sem((3, 3)), sem((3, 3)), sem((3, 2)), sem((3, 2)), sem((5,)), sem((3,)), sem((3,)), sem((3,)),
               sem((RING,)), sem((GROUPS,)), sem((2, GROUPS)), sem,
               sem((RING,)), sem((GROUPS,)), sem((3, GROUPS)), sem((2,)), sem, sem],
            compiler_params=pltpu.CompilerParams(collective_id=0, has_side_effects=True, vmem_limit_bytes=63 * 1024 * 1024),
            name="moe_layer",
        )(idx_t, gate_t, tokens, w_gate[0], w_up[0], w_down[0])
        return out

    return jax.shard_map(device_step, mesh=mesh, in_specs=(row_spec, row_spec, row_spec, P('ep', 'fsdp', None), P('ep', 'fsdp', None), P('ep', None, 'fsdp')), out_specs=row_spec, check_vma=False)
```

```python
import functools

import jax
import jax.numpy as jnp
from jax import lax
from jax.experimental import pallas as pl
from jax.experimental.pallas import tpu as pltpu
from jax.sharding import PartitionSpec as P

F32 = jnp.float32
BF16 = jnp.bfloat16
MESH = pl.DeviceIdType.MESH
SIDE = 4
STRIDE = (16, 4, 1)
N_EXP = 64
GROUPS, PER = 8, 8
ROUTES = ((2, 1, 0), (1, 0, 2), (0, 2, 1))
OUT_ROUTES = ((0, 1, 2), (1, 2, 0), (2, 0, 1))
LEAD = 3
RING = 3


def hits(idx_t, eid):
    hit = jnp.zeros((eid.shape[0], idx_t.shape[1]), F32)
    for j in range(6):
        hit = jnp.where(idx_t[j:j + 1, :] == eid, 1.0, hit)
    return hit


def slot_keys(hit, earlier):
    before = jnp.dot(hit.astype(BF16), earlier, preferred_element_type=F32)
    return jnp.where(hit > 0.5, before, -1.0)


def offset(g, i):
    dz, b = i // 2, i % 2
    fixed = isinstance(g, int)
    low, high = (g % 2, g // 2) if fixed else (lax.rem(g, 2), lax.div(g, 2))
    lean = 2 * b + low
    dy, dx = dz + lean, lean + high + SIDE - dz
    return (dz, dy % SIDE, dx % SIDE) if fixed else (dz, lax.rem(dy, SIDE), lax.rem(dx, SIDE))


def moved(d):
    return (d + SIDE - 1) // SIDE if isinstance(d, int) else lax.div(d + SIDE - 1, SIDE)


def if_moves(d, far, near=None):
    if isinstance(d, int):
        (far if d else near or (lambda: None))()
        return
    pl.when(d > 0)(far)
    if near is not None:
        pl.when(d == 0)(near)


def layer_kernel(cap, cuts, idx_hbm, gate_hbm, tok_ref, wg, wu, wd, out_ref, inbox, back,
                 wgu, wdn, toks_z, toks_y, toks_x, idx_all, gate_all, idx_ref, gate_ref, keys, gates, acc, partial, stage, xbuf, outs, land,
                 ag_send, ag_recv, ix_send, ix_recv, gt_send, gt_recv, on_send, on_recv, own_sem, w_loc, w_send, w_recv,
                 d_send, d_keep, d_recv, d_relay, c_send, c_keep, c_recv, c_relay, p_send, p_recv, x_sem, m_sem):
    tok, dim = acc.shape[1:]
    half, ffn = wg.shape
    rows = PER * cap
    far = rows // SIDE * (SIDE - 1)
    me = lax.axis_index('ep')
    core = lax.axis_index('fsdp')
    pos = (lax.div(me, 16), lax.rem(lax.div(me, 4), 4), lax.rem(me, 4))
    gathered = (toks_z, toks_y, toks_x)

    def shifted(a, k):
        return me + (lax.rem(pos[a] + k, SIDE) - pos[a]) * STRIDE[a]

    def ag_copies(a, k):
        dev = {'ep': shifted(a, k)}
        lo, hi = cuts[a], cuts[a + 1]
        yield pltpu.make_async_remote_copy(src_ref=idx_hbm, dst_ref=idx_all.at[a, k - 1], send_sem=ix_send.at[a, k - 1],
                                           recv_sem=ix_recv.at[a, k - 1], device_id=dev, device_id_type=MESH)
        yield pltpu.make_async_remote_copy(src_ref=gate_hbm, dst_ref=gate_all.at[a, k - 1], send_sem=gt_send.at[a, k - 1],
                                           recv_sem=gt_recv.at[a, k - 1], device_id=dev, device_id_type=MESH)
        if k != 2:
            yield pltpu.make_async_remote_copy(src_ref=tok_ref.at[:, pl.ds(lo, hi - lo)], dst_ref=gathered[a].at[k],
                                               send_sem=ag_send.at[a, k - 1], recv_sem=ag_recv.at[a, k - 1],
                                               device_id=dev, device_id_type=MESH)

    def pass_on(a, k):
        part = pl.ds(0 if k == 1 else tok // 2, tok // 2)
        return pltpu.make_async_remote_copy(src_ref=gathered[a].at[k, part], dst_ref=gathered[a].at[2, part],
                                            send_sem=on_send.at[a, k // 2], recv_sem=on_recv.at[a, k // 2],
                                            device_id={'ep': shifted(a, k)}, device_id_type=MESH)

    barrier = pltpu.get_barrier_semaphore()
    for a in range(3):
        for k in range(1, SIDE):
            pl.semaphore_signal(barrier, inc=1, device_id={'ep': shifted(a, k)}, device_id_type=MESH)
    pl.semaphore_signal(barrier, inc=1, device_id={'fsdp': 1 - core}, device_id_type=MESH)

    at = pl.ds(pl.multiple_of(core * half, half), half)
    spots = ((wg, wgu.at[at, pl.ds(0, ffn)]), (wu, wgu.at[at, pl.ds(ffn, ffn)]), (wd, wdn.at[:, at]))
    w_copies = []
    for n, (src, dst) in enumerate(spots):
        w_copies.append(pltpu.make_async_copy(src, dst, w_loc.at[n]))
        w_copies.append(pltpu.make_async_remote_copy(src_ref=src, dst_ref=dst, send_sem=w_send.at[n], recv_sem=w_recv.at[n],
                                                     device_id={'fsdp': 1 - core}, device_id_type=MESH))

    own = [pltpu.make_async_copy(tok_ref.at[:, pl.ds(cuts[a], cuts[a + 1] - cuts[a])], gathered[a].at[0], own_sem.at[a]) for a in range(3)]
    own += [pltpu.make_async_copy(idx_hbm, idx_ref, own_sem.at[3]), pltpu.make_async_copy(gate_hbm, gate_ref, own_sem.at[4])]
    for c in own[::-1]:
        c.start()
    pl.semaphore_wait(barrier, 10)
    for k in (1, 3, 2):
        for a in range(3):
            for c in ag_copies(a, k):
                c.start()
    for c in w_copies:
        c.start()

    before = lax.broadcasted_iota(jnp.int32, (tok, tok), 0)
    after = lax.broadcasted_iota(jnp.int32, (tok, tok), 1)
    earlier = jnp.where(before < after, 1.0, 0.0).astype(BF16)
    slot = lax.broadcasted_iota(jnp.int32, (cap, tok), 0).astype(F32)

    def block(i, p):
        return pl.ds(i * cap, cap), pl.ds(cuts[p], cuts[p + 1] - cuts[p])

    def each(g, routes):
        for i in range(PER):
            ds = offset(g, i)
            for p in range(3):
                yield i, p, [ds[axis] for axis in routes[p]]

    def wait_rows(ref, n, sem):
        part = ref.at[pl.ds(0, n)]
        pltpu.make_async_copy(part, part, sem).wait()

    def plane_keys(a, k):
        q = lax.broadcasted_iota(jnp.int32, (16, 1), 0)
        _, b, c = OUT_ROUTES[a]
        eid = pos[a] * STRIDE[a] + ((pos[b] + (q >> 2)) & 3) * STRIDE[b] + ((pos[c] + (q & 3)) & 3) * STRIDE[c]
        ids = idx_ref[...] if k == 0 else idx_all[a, k - 1]
        keys[a, k] = slot_keys(hits(ids, eid), earlier)
        gate = gate_ref[...] if k == 0 else gate_all[a, k - 1]
        mine = jnp.zeros((16, tok), F32)
        for j in range(6):
            mine = jnp.where(ids[j:j + 1, :] == eid, gate[j:j + 1, :], mine)
        gates[a, k] = mine

    def back_of(d):
        return (SIDE - d) % SIDE if isinstance(d, int) else lax.rem(SIDE - d, SIDE)

    def pick(g):
        ring = lax.rem(g, RING)

        @pl.when(g >= RING)
        def _():
            wait_rows(stage.at[ring], far, d_send.at[ring])

        pick_blocks(g, ring, list(each(g, OUT_ROUTES)))

    def pick_blocks(g, ring, blocks):
        for i, p, d in blocks:
            lo, hi = cuts[p], cuts[p + 1]
            k = back_of(d[0])
            key = keys[p, k, pl.ds(back_of(d[1]) * 4 + back_of(d[2]), 1), :]
            sel = jnp.where(key == slot, 1.0, 0.0).astype(BF16)
            got = jnp.dot(sel, gathered[p][k], preferred_element_type=F32)
            stage[ring, i * cap:(i + 1) * cap, lo:hi] = got.astype(BF16)
        for i, p, d in blocks:
            src, dst = stage.at[ring, *block(i, p)], inbox.at[0, g, *block(i, p)]
            if_moves(d[1], lambda: pltpu.make_async_remote_copy(
                src_ref=src, dst_ref=dst, send_sem=d_send.at[ring], recv_sem=d_recv.at[0, g],
                device_id={'ep': shifted(OUT_ROUTES[p][1], back_of(d[1]))}, device_id_type=MESH).start(),
                lambda: pltpu.make_async_copy(src, dst, d_keep.at[g]).start())

    def early_picks(k):
        for g in range(LEAD):
            pick_blocks(g, g, [(i, p, d) for i, p, d in each(g, OUT_ROUTES) if back_of(d[0]) == k])

    def forward(g):
        wait_rows(inbox.at[0, g], far, d_recv.at[0, g])
        wait_rows(inbox.at[0, g], rows - far, d_keep.at[g])
        for i, p, d in each(g, OUT_ROUTES):
            if_moves(d[2], lambda: pltpu.make_async_remote_copy(
                src_ref=inbox.at[0, g, *block(i, p)], dst_ref=inbox.at[1, g, *block(i, p)], send_sem=d_relay,
                recv_sem=d_recv.at[1, g], device_id={'ep': shifted(OUT_ROUTES[p][2], back_of(d[2]))}, device_id_type=MESH).start())

    def fetch(g):
        wait_rows(inbox.at[1, g], far, d_recv.at[1, g])
        for i, p, d in each(g, OUT_ROUTES):
            pltpu.make_async_copy(inbox.at[moved(d[2]), g, *block(i, p)], xbuf.at[block(i, p)], x_sem).start()

    def experts(g):
        ring = lax.rem(g, RING)
        pltpu.make_async_copy(xbuf, xbuf, x_sem).wait()

        @pl.when(g >= RING)
        def _():
            wait_rows(outs.at[ring], far, c_send.at[ring])

        both = jnp.dot(xbuf[...], wgu[...], preferred_element_type=F32)
        act_a, act_b = both[:, :ffn], both[:, ffn:]
        hidden = (act_a * jax.nn.sigmoid(act_a) * act_b).astype(BF16)
        outs[ring] = jnp.dot(hidden, wdn[...], preferred_element_type=F32).astype(BF16)
        for i, p, d in each(g, ROUTES):
            src = outs.at[ring, *block(i, p)]
            if_moves(d[0], lambda: hop(src, 0, g, i, p, d[0], c_send.at[ring]).start(),
                     lambda: pltpu.make_async_copy(src, back.at[0, g, *block(i, p)], c_keep.at[g]).start())

    def hop(src, leg, g, i, p, d, send):
        return pltpu.make_async_remote_copy(
            src_ref=src, dst_ref=back.at[leg, g, *block(i, p)], send_sem=send, recv_sem=c_recv.at[leg, g],
            device_id={'ep': shifted(ROUTES[p][leg], d)}, device_id_type=MESH)

    def second_hops(g):
        wait_rows(back.at[0, g], far, c_recv.at[0, g])
        wait_rows(back.at[0, g], rows - far, c_keep.at[g])
        for i, p, d in each(g, ROUTES):
            if_moves(d[1], lambda: hop(back.at[0, g, *block(i, p)], 1, g, i, p, d[1], c_relay).start())

    def partial_copy(p, d):
        span = pl.ds(cuts[p], cuts[p + 1] - cuts[p])
        return pltpu.make_async_remote_copy(
            src_ref=acc.at[d, :, span], dst_ref=partial.at[d - 1, :, span], send_sem=p_send.at[p, d - 1],
            recv_sem=p_recv.at[p, d - 1], device_id={'ep': shifted(ROUTES[p][2], d)}, device_id_type=MESH)

    def quarter(x):
        return x % SIDE if isinstance(x, int) else lax.rem(x + 2 * SIDE, SIDE)

    def members(m, p, d):
        for n in range(4):
            odd, b = n // 2, n % 2
            lean = 2 * b + odd
            axis = ROUTES[p][2]
            dz = d if axis == 0 else quarter(d - lean) if axis == 1 else quarter(lean + m - d)
            dy = d if axis == 1 else quarter(dz + lean)
            dx = d if axis == 2 else quarter(lean + m - dz)
            yield n, 2 * m + odd, 2 * dz + b, (dz, dy, dx)

    def mix(m):
        for odd in range(2):
            wait_rows(back.at[1, 2 * m + odd], far, c_recv.at[1, 2 * m + odd])
        for d in range(SIDE):
            for p in range(3):
                span = pl.ds(cuts[p], cuts[p + 1] - cuts[p])
                for n, g, i, ds in members(m, p, d):
                    start = i * cap if isinstance(i, int) else pl.multiple_of(i * cap, cap)
                    pltpu.make_async_copy(back.at[moved(ds[ROUTES[p][1]]), g, pl.ds(start, cap), span],
                                          land.at[pl.ds((4 * d + n) * cap, cap), span], m_sem).start()
        pltpu.make_async_copy(land, land, m_sem).wait()
        for d in (2, 1, 3, 0):
            for p in range(3):
                lo, hi = cuts[p], cuts[p + 1]
                a = ROUTES[p][2]
                _, b, c = OUT_ROUTES[a]
                tall = []
                for n, g, i, ds in members(m, p, d):
                    row = pl.ds(back_of(ds[b]) * 4 + back_of(ds[c]), 1)
                    here = keys[a, (SIDE - d) % SIDE, row, :] == slot
                    left = gates[a, (SIDE - d) % SIDE, row, :]
                    wide = []
                    for _ in range(3):
                        piece = left.astype(BF16).astype(F32)
                        left = left - piece
                        wide.append(jnp.where(here, piece, 0.0))
                    tall.append(jnp.concatenate(wide, axis=1))
                weight = jnp.concatenate(tall, axis=0).astype(BF16)
                parts = lax.dot_general(weight, land[4 * d * cap:4 * (d + 1) * cap, lo:hi], (((0,), (0,)), ((), ())),
                                        preferred_element_type=F32)
                acc[d, :, lo:hi] += parts[:tok] + parts[tok:2 * tok] + parts[2 * tok:]
            if d:
                @pl.when(m == GROUPS // 2 - 1)
                def _():
                    for p in range(3):
                        partial_copy(p, d).start()

    def mix_odd(g):
        pl.when(lax.rem(g, 2) == 1)(lambda: mix(lax.div(g, 2)))

    own[3].wait()
    own[4].wait()
    for a in range(3):
        plane_keys(a, 0)
        own[a].wait()
        acc[0, :, cuts[a]:cuts[a + 1]] = gathered[a][0].astype(F32)
    early_picks(0)
    acc[1:] = jnp.zeros((SIDE - 1, tok, dim), F32)
    for k in (1, 3):
        for a in range(3):
            for c in ag_copies(a, k):
                c.wait_recv()
            pass_on(a, k).start()
    for k in (1, 3, 2):
        for a in range(3):
            if k == 2:
                for c in ag_copies(a, k):
                    c.wait_recv()
                pass_on(a, 1).wait_recv()
                pass_on(a, 3).wait_recv()
            plane_keys(a, k)
        early_picks(k)
    for a in range(3):
        for k in (2, 1, 3):
            for c in ag_copies(a, k):
                c.wait_send()
        pass_on(a, 1).wait_send()
        pass_on(a, 3).wait_send()

    def in_turn(r, lag, step):
        g = r - lag
        pl.when((g >= 0) & (g < GROUPS))(lambda: step(g))

    @pl.loop(0, GROUPS + 3)
    def _(r):
        @pl.when(r == 1)
        def _():
            for c in w_copies:
                c.wait()

        in_turn(r, 0, forward)
        in_turn(r, 1, fetch)
        pl.when(r + LEAD < GROUPS)(lambda: pick(r + LEAD))
        in_turn(r, 1, experts)
        in_turn(r, 2, second_hops)
        in_turn(r, 3, mix_odd)

    for p in range(3):
        lo, hi = cuts[p], cuts[p + 1]
        for d in (1, 3, 2):
            partial_copy(p, d).wait()
        out_ref[:, lo:hi] = (acc[0, :, lo:hi] + partial[0, :, lo:hi] + partial[1, :, lo:hi] + partial[2, :, lo:hi]).astype(BF16)
    for ring in range(RING):
        wait_rows(stage.at[ring], far, d_send.at[ring])
        wait_rows(outs.at[ring], far, c_send.at[ring])
    for sem in (d_relay, c_relay):
        part = back.at[0, :, pl.ds(0, far)]
        pltpu.make_async_copy(part, part, sem).wait()


def solution(mesh):
    row_spec = P(('rep', 'ep', 'fsdp'), None)

    def device_step(tokens, expert_idx, gates, w_gate, w_up, w_down):
        tok, top_k = expert_idx.shape
        dim = tokens.shape[1]
        half, width = w_gate.shape[1:]
        cap = (2 * tok * top_k + N_EXP - 1) // N_EXP
        cuts = (0, 640, 1280, dim)
        rows = PER * cap
        idx_t = expert_idx.T
        gate_t = gates.T
        vmem = pl.BlockSpec(memory_space=pltpu.VMEM)
        hbm = pl.BlockSpec(memory_space=pl.ANY)
        sem = pltpu.SemaphoreType.DMA
        out, _, _ = pl.pallas_call(
            functools.partial(layer_kernel, cap, cuts),
            out_shape=(jax.ShapeDtypeStruct((tok, dim), BF16), jax.ShapeDtypeStruct((2, GROUPS, rows, dim), BF16),
                       jax.ShapeDtypeStruct((2, GROUPS, rows, dim), BF16)),
            in_specs=[hbm] * 6,
            out_specs=(vmem, hbm, hbm),
            scratch_shapes=[pltpu.VMEM((dim, 2 * width), BF16), pltpu.VMEM((width, dim), BF16)]
            + [pltpu.VMEM((SIDE, tok, cuts[a + 1] - cuts[a]), BF16) for a in range(3)]
            + [pltpu.VMEM((3, 3, top_k, tok), jnp.int32), pltpu.VMEM((3, 3, top_k, tok), F32), pltpu.VMEM((top_k, tok), jnp.int32), pltpu.VMEM((top_k, tok), F32), pltpu.VMEM((3, SIDE, 16, tok), F32), pltpu.VMEM((3, SIDE, 16, tok), F32),
               pltpu.VMEM((SIDE, tok, dim), F32), pltpu.VMEM((SIDE - 1, tok, dim), F32), pltpu.VMEM((RING, rows, dim), BF16),
               pltpu.VMEM((rows, dim), BF16), pltpu.VMEM((RING, rows, dim), BF16), pltpu.VMEM((2 * rows, dim), BF16),
               sem((3, 3)), sem((3, 3)), sem((3, 3)), sem((3, 3)), sem((3, 3)), sem((3, 3)), sem((3, 2)), sem((3, 2)), sem((5,)),
               sem((3,)), sem((3,)), sem((3,)),
               sem((RING,)), sem((GROUPS,)), sem((2, GROUPS)), sem,
               sem((RING,)), sem((GROUPS,)), sem((2, GROUPS)), sem, sem((3, 3)), sem((3, 3)), sem, sem],
            compiler_params=pltpu.CompilerParams(collective_id=0, has_side_effects=True, vmem_limit_bytes=63 * 1024 * 1024),
            name="moe_layer",
        )(idx_t, gate_t, tokens, w_gate[0], w_up[0], w_down[0])
        return out

    return jax.shard_map(device_step, mesh=mesh, in_specs=(row_spec, row_spec, row_spec, P('ep', 'fsdp', None), P('ep', 'fsdp', None), P('ep', None, 'fsdp')), out_specs=row_spec, check_vma=False)
```

```python
import functools

import jax
import jax.numpy as jnp
from jax import lax
from jax.experimental import pallas as pl
from jax.experimental.pallas import tpu as pltpu
from jax.sharding import PartitionSpec as P

F32 = jnp.float32
BF16 = jnp.bfloat16
MESH = pl.DeviceIdType.MESH
SIDE = 4
STRIDE = (16, 4, 1)
N_EXP = 64
GROUPS, PER = 8, 8
ROUTES = ((2, 1, 0), (1, 0, 2), (0, 2, 1))
OUT_ROUTES = ((0, 1, 2), (1, 2, 0), (2, 0, 1))
LEAD = 3
RING = 3


def hits(idx_t, eid):
    hit = jnp.zeros((eid.shape[0], idx_t.shape[1]), F32)
    for j in range(6):
        hit = jnp.where(idx_t[j:j + 1, :] == eid, 1.0, hit)
    return hit


def slot_keys(hit, earlier):
    before = jnp.dot(hit.astype(BF16), earlier, preferred_element_type=F32)
    return jnp.where(hit > 0.5, before, -1.0)


def offset(g, i):
    dz, b = i // 2, i % 2
    fixed = isinstance(g, int)
    low, high = (g % 2, g // 2) if fixed else (lax.rem(g, 2), lax.div(g, 2))
    lean = 2 * b + low
    dy, dx = dz + lean, lean + high + SIDE - dz
    return (dz, dy % SIDE, dx % SIDE) if fixed else (dz, lax.rem(dy, SIDE), lax.rem(dx, SIDE))


def moved(d):
    return (d + SIDE - 1) // SIDE if isinstance(d, int) else lax.div(d + SIDE - 1, SIDE)


def if_moves(d, far, near=None):
    if isinstance(d, int):
        (far if d else near or (lambda: None))()
        return
    pl.when(d > 0)(far)
    if near is not None:
        pl.when(d == 0)(near)


def layer_kernel(cap, cuts, idx_hbm, gate_hbm, tok_ref, wg, wu, wd, out_ref, inbox, back,
                 wgu, wdn, toks_z, toks_y, toks_x, idx_all, gate_all, idx_ref, gate_ref, keys, gates, acc, partial, stage, xbuf, outs, land,
                 ag_send, ag_recv, ix_send, ix_recv, gt_send, gt_recv, on_send, on_recv, own_sem, w_loc, w_send, w_recv,
                 d_send, d_keep, d_recv, d_relay, c_send, c_keep, c_recv, c_relay, j_send, j_recv, p_send, p_recv, x_sem, m_sem):
    tok, dim = acc.shape[1:]
    half, ffn = wg.shape
    rows = PER * cap
    far = rows // SIDE * (SIDE - 1)
    me = lax.axis_index('ep')
    core = lax.axis_index('fsdp')
    pos = (lax.div(me, 16), lax.rem(lax.div(me, 4), 4), lax.rem(me, 4))
    gathered = (toks_z, toks_y, toks_x)

    def shifted(a, k):
        return me + (lax.rem(pos[a] + k, SIDE) - pos[a]) * STRIDE[a]

    def ag_copies(a, k):
        dev = {'ep': shifted(a, k)}
        lo, hi = cuts[a], cuts[a + 1]
        yield pltpu.make_async_remote_copy(src_ref=idx_hbm, dst_ref=idx_all.at[a, k - 1], send_sem=ix_send.at[a, k - 1],
                                           recv_sem=ix_recv.at[a, k - 1], device_id=dev, device_id_type=MESH)
        yield pltpu.make_async_remote_copy(src_ref=gate_hbm, dst_ref=gate_all.at[a, k - 1], send_sem=gt_send.at[a, k - 1],
                                           recv_sem=gt_recv.at[a, k - 1], device_id=dev, device_id_type=MESH)
        if k != 2:
            yield pltpu.make_async_remote_copy(src_ref=tok_ref.at[:, pl.ds(lo, hi - lo)], dst_ref=gathered[a].at[k],
                                               send_sem=ag_send.at[a, k - 1], recv_sem=ag_recv.at[a, k - 1],
                                               device_id=dev, device_id_type=MESH)

    def pass_on(a, k):
        part = pl.ds(0 if k == 1 else tok // 2, tok // 2)
        return pltpu.make_async_remote_copy(src_ref=gathered[a].at[k, part], dst_ref=gathered[a].at[2, part],
                                            send_sem=on_send.at[a, k // 2], recv_sem=on_recv.at[a, k // 2],
                                            device_id={'ep': shifted(a, k)}, device_id_type=MESH)

    barrier = pltpu.get_barrier_semaphore()
    for a in range(3):
        for k in range(1, SIDE):
            pl.semaphore_signal(barrier, inc=1, device_id={'ep': shifted(a, k)}, device_id_type=MESH)
    pl.semaphore_signal(barrier, inc=1, device_id={'fsdp': 1 - core}, device_id_type=MESH)

    at = pl.ds(pl.multiple_of(core * half, half), half)
    spots = ((wg, wgu.at[at, pl.ds(0, ffn)]), (wu, wgu.at[at, pl.ds(ffn, ffn)]), (wd, wdn.at[:, at]))
    w_copies = []
    for n, (src, dst) in enumerate(spots):
        w_copies.append(pltpu.make_async_copy(src, dst, w_loc.at[n]))
        w_copies.append(pltpu.make_async_remote_copy(src_ref=src, dst_ref=dst, send_sem=w_send.at[n], recv_sem=w_recv.at[n],
                                                     device_id={'fsdp': 1 - core}, device_id_type=MESH))

    own = [pltpu.make_async_copy(tok_ref.at[:, pl.ds(cuts[a], cuts[a + 1] - cuts[a])], gathered[a].at[0], own_sem.at[a]) for a in range(3)]
    own += [pltpu.make_async_copy(idx_hbm, idx_ref, own_sem.at[3]), pltpu.make_async_copy(gate_hbm, gate_ref, own_sem.at[4])]
    for c in own[::-1]:
        c.start()
    pl.semaphore_wait(barrier, 10)
    for k in (1, 3, 2):
        for a in range(3):
            for c in ag_copies(a, k):
                c.start()
    for c in w_copies:
        c.start()

    before = lax.broadcasted_iota(jnp.int32, (tok, tok), 0)
    after = lax.broadcasted_iota(jnp.int32, (tok, tok), 1)
    earlier = jnp.where(before < after, 1.0, 0.0).astype(BF16)
    slot = lax.broadcasted_iota(jnp.int32, (cap, tok), 0).astype(F32)

    def block(i, p):
        return pl.ds(i * cap, cap), pl.ds(cuts[p], cuts[p + 1] - cuts[p])

    def each(g, routes):
        for i in range(PER):
            ds = offset(g, i)
            for p in range(3):
                yield i, p, [ds[axis] for axis in routes[p]]

    def wait_rows(ref, n, sem):
        part = ref.at[pl.ds(0, n)]
        pltpu.make_async_copy(part, part, sem).wait()

    def plane_keys(a, k):
        q = lax.broadcasted_iota(jnp.int32, (16, 1), 0)
        _, b, c = OUT_ROUTES[a]
        eid = pos[a] * STRIDE[a] + ((pos[b] + (q >> 2)) & 3) * STRIDE[b] + ((pos[c] + (q & 3)) & 3) * STRIDE[c]
        ids = idx_ref[...] if k == 0 else idx_all[a, k - 1]
        keys[a, k] = slot_keys(hits(ids, eid), earlier)
        gate = gate_ref[...] if k == 0 else gate_all[a, k - 1]
        mine = jnp.zeros((16, tok), F32)
        for j in range(6):
            mine = jnp.where(ids[j:j + 1, :] == eid, gate[j:j + 1, :], mine)
        gates[a, k] = mine

    def back_of(d):
        return (SIDE - d) % SIDE if isinstance(d, int) else lax.rem(SIDE - d, SIDE)

    def pick(g):
        ring = lax.rem(g, RING)

        @pl.when(g >= RING)
        def _():
            wait_rows(stage.at[ring], far, d_send.at[ring])

        pick_blocks(g, ring, list(each(g, OUT_ROUTES)))

    def pick_blocks(g, ring, blocks):
        for i, p, d in blocks:
            lo, hi = cuts[p], cuts[p + 1]
            k = back_of(d[0])
            key = keys[p, k, pl.ds(back_of(d[1]) * 4 + back_of(d[2]), 1), :]
            sel = jnp.where(key == slot, 1.0, 0.0).astype(BF16)
            got = jnp.dot(sel, gathered[p][k], preferred_element_type=F32)
            stage[ring, i * cap:(i + 1) * cap, lo:hi] = got.astype(BF16)
        for i, p, d in blocks:
            src, dst = stage.at[ring, *block(i, p)], inbox.at[0, g, *block(i, p)]
            if_moves(d[1], lambda: pltpu.make_async_remote_copy(
                src_ref=src, dst_ref=dst, send_sem=d_send.at[ring], recv_sem=d_recv.at[0, g],
                device_id={'ep': shifted(OUT_ROUTES[p][1], back_of(d[1]))}, device_id_type=MESH).start(),
                lambda: pltpu.make_async_copy(src, dst, d_keep.at[g]).start())

    def early_picks(k):
        for g in range(LEAD):
            pick_blocks(g, g, [(i, p, d) for i, p, d in each(g, OUT_ROUTES) if back_of(d[0]) == k])

    def forward(g):
        wait_rows(inbox.at[0, g], far, d_recv.at[0, g])
        wait_rows(inbox.at[0, g], rows - far, d_keep.at[g])
        for i, p, d in each(g, OUT_ROUTES):
            if_moves(d[2], lambda: pltpu.make_async_remote_copy(
                src_ref=inbox.at[0, g, *block(i, p)], dst_ref=inbox.at[1, g, *block(i, p)], send_sem=d_relay,
                recv_sem=d_recv.at[1, g], device_id={'ep': shifted(OUT_ROUTES[p][2], back_of(d[2]))}, device_id_type=MESH).start())

    def fetch(g):
        wait_rows(inbox.at[1, g], far, d_recv.at[1, g])
        for i, p, d in each(g, OUT_ROUTES):
            pltpu.make_async_copy(inbox.at[moved(d[2]), g, *block(i, p)], xbuf.at[block(i, p)], x_sem).start()

    def experts(g):
        ring = lax.rem(g, RING)
        pltpu.make_async_copy(xbuf, xbuf, x_sem).wait()

        @pl.when(g >= RING)
        def _():
            wait_rows(outs.at[ring], far, c_send.at[ring])

        both = jnp.dot(xbuf[...], wgu[...], preferred_element_type=F32)
        act_a, act_b = both[:, :ffn], both[:, ffn:]
        hidden = (act_a * jax.nn.sigmoid(act_a) * act_b).astype(BF16)
        outs[ring] = jnp.dot(hidden, wdn[...], preferred_element_type=F32).astype(BF16)
        for i, p, d in each(g, ROUTES):
            src = outs.at[ring, *block(i, p)]
            if_moves(d[0], lambda: hop(src, 0, g, i, p, d[0], c_send.at[ring]).start(),
                     lambda: pltpu.make_async_copy(src, back.at[0, g, *block(i, p)], c_keep.at[g]).start())

    def hop(src, leg, g, i, p, d, send):
        return pltpu.make_async_remote_copy(
            src_ref=src, dst_ref=back.at[leg, g, *block(i, p)], send_sem=send, recv_sem=c_recv.at[leg, g],
            device_id={'ep': shifted(ROUTES[p][leg], d)}, device_id_type=MESH)

    def second_hops(g):
        wait_rows(back.at[0, g], far, c_recv.at[0, g])
        wait_rows(back.at[0, g], rows - far, c_keep.at[g])
        for i, p, d in each(g, ROUTES):
            if_moves(d[1], lambda: hop(back.at[0, g, *block(i, p)], 1, g, i, p, d[1], c_relay).start())

    def partial_copy(p, d, part):
        where = (pl.ds(part * (tok // 2), tok // 2), pl.ds(cuts[p], cuts[p + 1] - cuts[p]))
        if d == 2:
            step, sems = (1, 3)[part], (j_send.at[p, part], j_recv.at[p, part])
        else:
            step, sems = d, (p_send.at[p, d // 2, part], p_recv.at[p, d // 2, part])
        return pltpu.make_async_remote_copy(
            src_ref=acc.at[d, *where], dst_ref=partial.at[d - 1, *where], send_sem=sems[0], recv_sem=sems[1],
            device_id={'ep': shifted(ROUTES[p][2], step)}, device_id_type=MESH)

    def join(p):
        lo, hi = cuts[p], cuts[p + 1]
        for part, d in ((0, 1), (1, 3)):
            span = slice(part * (tok // 2), (part + 1) * (tok // 2))
            partial_copy(p, 2, part).wait_recv()
            acc[d, span, lo:hi] += partial[1, span, lo:hi]
            partial_copy(p, d, part).start()

    def quarter(x):
        return x % SIDE if isinstance(x, int) else lax.rem(x + 2 * SIDE, SIDE)

    def members(m, p, d):
        for n in range(4):
            odd, b = n // 2, n % 2
            lean = 2 * b + odd
            axis = ROUTES[p][2]
            dz = d if axis == 0 else quarter(d - lean) if axis == 1 else quarter(lean + m - d)
            dy = d if axis == 1 else quarter(dz + lean)
            dx = d if axis == 2 else quarter(lean + m - dz)
            yield n, 2 * m + odd, 2 * dz + b, (dz, dy, dx)

    def mix(m):
        for odd in range(2):
            wait_rows(back.at[1, 2 * m + odd], far, c_recv.at[1, 2 * m + odd])
        for d in range(SIDE):
            for p in range(3):
                span = pl.ds(cuts[p], cuts[p + 1] - cuts[p])
                for n, g, i, ds in members(m, p, d):
                    start = i * cap if isinstance(i, int) else pl.multiple_of(i * cap, cap)
                    pltpu.make_async_copy(back.at[moved(ds[ROUTES[p][1]]), g, pl.ds(start, cap), span],
                                          land.at[pl.ds((4 * d + n) * cap, cap), span], m_sem).start()
        pltpu.make_async_copy(land, land, m_sem).wait()
        for d in (2, 1, 3, 0):
            for p in range(3):
                lo, hi = cuts[p], cuts[p + 1]
                a = ROUTES[p][2]
                _, b, c = OUT_ROUTES[a]
                tall = []
                for n, g, i, ds in members(m, p, d):
                    row = pl.ds(back_of(ds[b]) * 4 + back_of(ds[c]), 1)
                    here = keys[a, (SIDE - d) % SIDE, row, :] == slot
                    left = gates[a, (SIDE - d) % SIDE, row, :]
                    wide = []
                    for _ in range(3):
                        piece = left.astype(BF16).astype(F32)
                        left = left - piece
                        wide.append(jnp.where(here, piece, 0.0))
                    tall.append(jnp.concatenate(wide, axis=1))
                weight = jnp.concatenate(tall, axis=0).astype(BF16)
                parts = lax.dot_general(weight, land[4 * d * cap:4 * (d + 1) * cap, lo:hi], (((0,), (0,)), ((), ())),
                                        preferred_element_type=F32)
                acc[d, :, lo:hi] += parts[:tok] + parts[tok:2 * tok] + parts[2 * tok:]
            if d:
                @pl.when(m == GROUPS // 2 - 1)
                def _():
                    for p in range(3):
                        for part in ((0, 1) if d == 2 else (1,) if d == 1 else (0,)):
                            partial_copy(p, d, part).start()

    def mix_odd(g):
        pl.when(lax.rem(g, 2) == 1)(lambda: mix(lax.div(g, 2)))

    own[3].wait()
    own[4].wait()
    for a in range(3):
        plane_keys(a, 0)
        own[a].wait()
        acc[0, :, cuts[a]:cuts[a + 1]] = gathered[a][0].astype(F32)
    early_picks(0)
    acc[1:] = jnp.zeros((SIDE - 1, tok, dim), F32)
    for k in (1, 3):
        for a in range(3):
            for c in ag_copies(a, k):
                c.wait_recv()
            pass_on(a, k).start()
    for k in (1, 3, 2):
        for a in range(3):
            if k == 2:
                for c in ag_copies(a, k):
                    c.wait_recv()
                pass_on(a, 1).wait_recv()
                pass_on(a, 3).wait_recv()
            plane_keys(a, k)
        early_picks(k)
    for a in range(3):
        for k in (2, 1, 3):
            for c in ag_copies(a, k):
                c.wait_send()
        pass_on(a, 1).wait_send()
        pass_on(a, 3).wait_send()

    def in_turn(r, lag, step):
        g = r - lag
        pl.when((g >= 0) & (g < GROUPS))(lambda: step(g))

    @pl.loop(0, GROUPS + 3)
    def _(r):
        @pl.when(r == 1)
        def _():
            for c in w_copies:
                c.wait()

        in_turn(r, 0, forward)
        in_turn(r, 1, fetch)
        pl.when(r + LEAD < GROUPS)(lambda: pick(r + LEAD))
        in_turn(r, 1, experts)
        in_turn(r, 2, second_hops)
        in_turn(r, 3, mix_odd)

    for p in range(3):
        join(p)
    for p in range(3):
        lo, hi = cuts[p], cuts[p + 1]
        for part in range(2):
            partial_copy(p, 2, part).wait_send()
            for d in (1, 3):
                partial_copy(p, d, part).wait()
        out_ref[:, lo:hi] = (acc[0, :, lo:hi] + partial[0, :, lo:hi] + partial[2, :, lo:hi]).astype(BF16)
    for ring in range(RING):
        wait_rows(stage.at[ring], far, d_send.at[ring])
        wait_rows(outs.at[ring], far, c_send.at[ring])
    for sem in (d_relay, c_relay):
        part = back.at[0, :, pl.ds(0, far)]
        pltpu.make_async_copy(part, part, sem).wait()


def solution(mesh):
    row_spec = P(('rep', 'ep', 'fsdp'), None)

    def device_step(tokens, expert_idx, gates, w_gate, w_up, w_down):
        tok, top_k = expert_idx.shape
        dim = tokens.shape[1]
        half, width = w_gate.shape[1:]
        cap = (2 * tok * top_k + N_EXP - 1) // N_EXP
        cuts = (0, 640, 1280, dim)
        rows = PER * cap
        idx_t = expert_idx.T
        gate_t = gates.T
        vmem = pl.BlockSpec(memory_space=pltpu.VMEM)
        hbm = pl.BlockSpec(memory_space=pl.ANY)
        sem = pltpu.SemaphoreType.DMA
        out, _, _ = pl.pallas_call(
            functools.partial(layer_kernel, cap, cuts),
            out_shape=(jax.ShapeDtypeStruct((tok, dim), BF16), jax.ShapeDtypeStruct((2, GROUPS, rows, dim), BF16),
                       jax.ShapeDtypeStruct((2, GROUPS, rows, dim), BF16)),
            in_specs=[hbm] * 6,
            out_specs=(vmem, hbm, hbm),
            scratch_shapes=[pltpu.VMEM((dim, 2 * width), BF16), pltpu.VMEM((width, dim), BF16)]
            + [pltpu.VMEM((SIDE, tok, cuts[a + 1] - cuts[a]), BF16) for a in range(3)]
            + [pltpu.VMEM((3, 3, top_k, tok), jnp.int32), pltpu.VMEM((3, 3, top_k, tok), F32), pltpu.VMEM((top_k, tok), jnp.int32), pltpu.VMEM((top_k, tok), F32), pltpu.VMEM((3, SIDE, 16, tok), F32), pltpu.VMEM((3, SIDE, 16, tok), F32),
               pltpu.VMEM((SIDE, tok, dim), F32), pltpu.VMEM((SIDE - 1, tok, dim), F32), pltpu.VMEM((RING, rows, dim), BF16),
               pltpu.VMEM((rows, dim), BF16), pltpu.VMEM((RING, rows, dim), BF16), pltpu.VMEM((2 * rows, dim), BF16),
               sem((3, 3)), sem((3, 3)), sem((3, 3)), sem((3, 3)), sem((3, 3)), sem((3, 3)), sem((3, 2)), sem((3, 2)), sem((5,)),
               sem((3,)), sem((3,)), sem((3,)),
               sem((RING,)), sem((GROUPS,)), sem((2, GROUPS)), sem,
               sem((RING,)), sem((GROUPS,)), sem((2, GROUPS)), sem, sem((3, 2)), sem((3, 2)), sem((3, 2, 2)), sem((3, 2, 2)), sem, sem],
            compiler_params=pltpu.CompilerParams(collective_id=0, has_side_effects=True, vmem_limit_bytes=63 * 1024 * 1024),
            name="moe_layer",
        )(idx_t, gate_t, tokens, w_gate[0], w_up[0], w_down[0])
        return out

    return jax.shard_map(device_step, mesh=mesh, in_specs=(row_spec, row_spec, row_spec, P('ep', 'fsdp', None), P('ep', 'fsdp', None), P('ep', None, 'fsdp')), out_specs=row_spec, check_vma=False)
```

```python
import functools

import jax
import jax.numpy as jnp
from jax import lax
from jax.experimental import pallas as pl
from jax.experimental.pallas import tpu as pltpu
from jax.sharding import PartitionSpec as P

F32 = jnp.float32
BF16 = jnp.bfloat16
MESH = pl.DeviceIdType.MESH
SIDE = 4
STRIDE = (16, 4, 1)
N_EXP = 64
GROUPS, PER = 8, 8
ROUTES = ((2, 1, 0), (1, 0, 2), (0, 2, 1))
OUT_ROUTES = ((0, 1, 2), (1, 2, 0), (2, 0, 1))
LEAD = 3
RING = 3


def hits(idx_t, eid):
    hit = jnp.zeros((eid.shape[0], idx_t.shape[1]), F32)
    for j in range(6):
        hit = jnp.where(idx_t[j:j + 1, :] == eid, 1.0, hit)
    return hit


def slot_keys(hit, earlier):
    before = jnp.dot(hit.astype(BF16), earlier, preferred_element_type=F32)
    return jnp.where(hit > 0.5, before, -1.0)


def offset(g, i):
    dz, b = i // 2, i % 2
    fixed = isinstance(g, int)
    low, high = (g % 2, g // 2) if fixed else (lax.rem(g, 2), lax.div(g, 2))
    lean = 2 * b + low
    dy, dx = dz + lean, lean + high + SIDE - dz
    return (dz, dy % SIDE, dx % SIDE) if fixed else (dz, lax.rem(dy, SIDE), lax.rem(dx, SIDE))


def moved(d):
    return (d + SIDE - 1) // SIDE if isinstance(d, int) else lax.div(d + SIDE - 1, SIDE)


def if_moves(d, far, near=None):
    if isinstance(d, int):
        (far if d else near or (lambda: None))()
        return
    pl.when(d > 0)(far)
    if near is not None:
        pl.when(d == 0)(near)


def layer_kernel(cap, cuts, idx_hbm, gate_hbm, tok_ref, wg, wu, wd, out_ref, inbox, back,
                 wgu, wdn, toks_z, toks_y, toks_x, idx_all, gate_all, idx_ref, gate_ref, keys, gates, acc, partial, stage, xbuf, outs, land,
                 ag_send, ag_recv, ix_send, ix_recv, gt_send, gt_recv, on_send, on_recv, own_sem, w_loc, w_send, w_recv,
                 d_send, d_keep, d_recv, d_relay, c_send, c_keep, c_recv, c_relay, j_send, j_recv, p_send, p_recv, x_sem, m_sem):
    tok, dim = acc.shape[1:]
    half, ffn = wg.shape
    rows = PER * cap
    far = rows // SIDE * (SIDE - 1)
    me = lax.axis_index('ep')
    core = lax.axis_index('fsdp')
    pos = (lax.div(me, 16), lax.rem(lax.div(me, 4), 4), lax.rem(me, 4))
    gathered = (toks_z, toks_y, toks_x)

    def shifted(a, k):
        return me + (lax.rem(pos[a] + k, SIDE) - pos[a]) * STRIDE[a]

    def ag_copies(a, k):
        dev = {'ep': shifted(a, k)}
        lo, hi = cuts[a], cuts[a + 1]
        yield pltpu.make_async_remote_copy(src_ref=idx_hbm, dst_ref=idx_all.at[a, k - 1], send_sem=ix_send.at[a, k - 1],
                                           recv_sem=ix_recv.at[a, k - 1], device_id=dev, device_id_type=MESH)
        yield pltpu.make_async_remote_copy(src_ref=gate_hbm, dst_ref=gate_all.at[a, k - 1], send_sem=gt_send.at[a, k - 1],
                                           recv_sem=gt_recv.at[a, k - 1], device_id=dev, device_id_type=MESH)
        if k != 2:
            yield pltpu.make_async_remote_copy(src_ref=tok_ref.at[:, pl.ds(lo, hi - lo)], dst_ref=gathered[a].at[k],
                                               send_sem=ag_send.at[a, k - 1], recv_sem=ag_recv.at[a, k - 1],
                                               device_id=dev, device_id_type=MESH)

    def pass_on(a, k):
        part = pl.ds(0 if k == 1 else tok // 2, tok // 2)
        return pltpu.make_async_remote_copy(src_ref=gathered[a].at[k, part], dst_ref=gathered[a].at[2, part],
                                            send_sem=on_send.at[a, k // 2], recv_sem=on_recv.at[a, k // 2],
                                            device_id={'ep': shifted(a, k)}, device_id_type=MESH)

    barrier = pltpu.get_barrier_semaphore()
    for a in range(3):
        for k in range(1, SIDE):
            pl.semaphore_signal(barrier, inc=1, device_id={'ep': shifted(a, k)}, device_id_type=MESH)
    pl.semaphore_signal(barrier, inc=1, device_id={'fsdp': 1 - core}, device_id_type=MESH)

    at = pl.ds(pl.multiple_of(core * half, half), half)
    spots = ((wg, wgu.at[at, pl.ds(0, ffn)]), (wu, wgu.at[at, pl.ds(ffn, ffn)]), (wd, wdn.at[:, at]))
    w_copies = []
    for n, (src, dst) in enumerate(spots):
        w_copies.append(pltpu.make_async_copy(src, dst, w_loc.at[n]))
        w_copies.append(pltpu.make_async_remote_copy(src_ref=src, dst_ref=dst, send_sem=w_send.at[n], recv_sem=w_recv.at[n],
                                                     device_id={'fsdp': 1 - core}, device_id_type=MESH))

    own = [pltpu.make_async_copy(tok_ref.at[:, pl.ds(cuts[a], cuts[a + 1] - cuts[a])], gathered[a].at[0], own_sem.at[a]) for a in range(3)]
    own += [pltpu.make_async_copy(idx_hbm, idx_ref, own_sem.at[3]), pltpu.make_async_copy(gate_hbm, gate_ref, own_sem.at[4])]
    for c in own[::-1]:
        c.start()
    pl.semaphore_wait(barrier, 10)
    for k in (1, 3, 2):
        for a in range(3):
            for c in ag_copies(a, k):
                c.start()
    for c in w_copies:
        c.start()

    before = lax.broadcasted_iota(jnp.int32, (tok, tok), 0)
    after = lax.broadcasted_iota(jnp.int32, (tok, tok), 1)
    earlier = jnp.where(before < after, 1.0, 0.0).astype(BF16)
    slot = lax.broadcasted_iota(jnp.int32, (cap, tok), 0).astype(F32)

    def block(i, p):
        return pl.ds(i * cap, cap), pl.ds(cuts[p], cuts[p + 1] - cuts[p])

    def each(g, routes):
        for i in range(PER):
            ds = offset(g, i)
            for p in range(3):
                yield i, p, [ds[axis] for axis in routes[p]]

    def wait_rows(ref, n, sem):
        part = ref.at[pl.ds(0, n)]
        pltpu.make_async_copy(part, part, sem).wait()

    def plane_keys(a, k):
        q = lax.broadcasted_iota(jnp.int32, (16, 1), 0)
        _, b, c = OUT_ROUTES[a]
        eid = pos[a] * STRIDE[a] + ((pos[b] + (q >> 2)) & 3) * STRIDE[b] + ((pos[c] + (q & 3)) & 3) * STRIDE[c]
        ids = idx_ref[...] if k == 0 else idx_all[a, k - 1]
        keys[a, k] = slot_keys(hits(ids, eid), earlier)
        gate = gate_ref[...] if k == 0 else gate_all[a, k - 1]
        mine = jnp.zeros((16, tok), F32)
        for j in range(6):
            mine = jnp.where(ids[j:j + 1, :] == eid, gate[j:j + 1, :], mine)
        gates[a, k] = mine

    def back_of(d):
        return (SIDE - d) % SIDE if isinstance(d, int) else lax.rem(SIDE - d, SIDE)

    def pick(g):
        ring = lax.rem(g, RING)

        @pl.when(g >= RING)
        def _():
            wait_rows(stage.at[ring], far, d_send.at[ring])

        pick_blocks(g, ring, list(each(g, OUT_ROUTES)))

    def pick_blocks(g, ring, blocks):
        for i, p, d in blocks:
            lo, hi = cuts[p], cuts[p + 1]
            k = back_of(d[0])
            key = keys[p, k, pl.ds(back_of(d[1]) * 4 + back_of(d[2]), 1), :]
            sel = jnp.where(key == slot, 1.0, 0.0).astype(BF16)
            got = jnp.dot(sel, gathered[p][k], preferred_element_type=F32)
            stage[ring, i * cap:(i + 1) * cap, lo:hi] = got.astype(BF16)
        for i, p, d in blocks:
            src, dst = stage.at[ring, *block(i, p)], inbox.at[0, g, *block(i, p)]
            if_moves(d[1], lambda: pltpu.make_async_remote_copy(
                src_ref=src, dst_ref=dst, send_sem=d_send.at[ring], recv_sem=d_recv.at[0, g],
                device_id={'ep': shifted(OUT_ROUTES[p][1], back_of(d[1]))}, device_id_type=MESH).start(),
                lambda: pltpu.make_async_copy(src, dst, d_keep.at[g]).start())

    def early_picks(k):
        for g in range(LEAD):
            pick_blocks(g, g, [(i, p, d) for i, p, d in each(g, OUT_ROUTES) if back_of(d[0]) == k])

    def forward(g):
        wait_rows(inbox.at[0, g], far, d_recv.at[0, g])
        wait_rows(inbox.at[0, g], rows - far, d_keep.at[g])
        for i, p, d in each(g, OUT_ROUTES):
            if_moves(d[2], lambda: pltpu.make_async_remote_copy(
                src_ref=inbox.at[0, g, *block(i, p)], dst_ref=inbox.at[1, g, *block(i, p)], send_sem=d_relay,
                recv_sem=d_recv.at[1, g], device_id={'ep': shifted(OUT_ROUTES[p][2], back_of(d[2]))}, device_id_type=MESH).start())

    def fetch(g):
        wait_rows(inbox.at[1, g], far, d_recv.at[1, g])
        for i, p, d in each(g, OUT_ROUTES):
            pltpu.make_async_copy(inbox.at[moved(d[2]), g, *block(i, p)], xbuf.at[block(i, p)], x_sem).start()

    def experts(g):
        ring = lax.rem(g, RING)
        pltpu.make_async_copy(xbuf, xbuf, x_sem).wait()

        @pl.when(g >= RING)
        def _():
            wait_rows(outs.at[ring], far, c_send.at[ring])

        both = jnp.dot(xbuf[...], wgu[...], preferred_element_type=F32)
        act_a, act_b = both[:, :ffn], both[:, ffn:]
        hidden = (act_a * jax.nn.sigmoid(act_a) * act_b).astype(BF16)
        outs[ring] = jnp.dot(hidden, wdn[...], preferred_element_type=F32).astype(BF16)
        for i, p, d in each(g, ROUTES):
            src = outs.at[ring, *block(i, p)]
            if_moves(d[0], lambda: hop(src, 0, g, i, p, d[0], c_send.at[ring]).start(),
                     lambda: pltpu.make_async_copy(src, back.at[0, g, *block(i, p)], c_keep.at[g]).start())

    def hop(src, leg, g, i, p, d, send):
        return pltpu.make_async_remote_copy(
            src_ref=src, dst_ref=back.at[leg, g, *block(i, p)], send_sem=send, recv_sem=c_recv.at[leg, g],
            device_id={'ep': shifted(ROUTES[p][leg], d)}, device_id_type=MESH)

    def second_hops(g):
        wait_rows(back.at[0, g], far, c_recv.at[0, g])
        wait_rows(back.at[0, g], rows - far, c_keep.at[g])
        for i, p, d in each(g, ROUTES):
            if_moves(d[1], lambda: hop(back.at[0, g, *block(i, p)], 1, g, i, p, d[1], c_relay).start())

    def partial_copy(p, d, part):
        where = (pl.ds(part * (tok // 2), tok // 2), pl.ds(cuts[p], cuts[p + 1] - cuts[p]))
        if d == 2:
            step, sems = (1, 3)[part], (j_send.at[p, part], j_recv.at[p, part])
        else:
            step, sems = d, (p_send.at[p, d // 2, part], p_recv.at[p, d // 2, part])
        return pltpu.make_async_remote_copy(
            src_ref=acc.at[d, *where], dst_ref=partial.at[d - 1, *where], send_sem=sems[0], recv_sem=sems[1],
            device_id={'ep': shifted(ROUTES[p][2], step)}, device_id_type=MESH)

    def join(p):
        lo, hi = cuts[p], cuts[p + 1]
        for part, d in ((0, 1), (1, 3)):
            span = slice(part * (tok // 2), (part + 1) * (tok // 2))
            partial_copy(p, 2, part).wait_recv()
            acc[d, span, lo:hi] += partial[1, span, lo:hi]
            partial_copy(p, d, part).start()

    def quarter(x):
        return x % SIDE if isinstance(x, int) else lax.rem(x + 2 * SIDE, SIDE)

    def members(m, p, d):
        for n in range(4):
            odd, b = n // 2, n % 2
            lean = 2 * b + odd
            axis = ROUTES[p][2]
            dz = d if axis == 0 else quarter(d - lean) if axis == 1 else quarter(lean + m - d)
            dy = d if axis == 1 else quarter(dz + lean)
            dx = d if axis == 2 else quarter(lean + m - dz)
            yield n, 2 * m + odd, 2 * dz + b, (dz, dy, dx)

    def mix(m):
        for odd in range(2):
            wait_rows(back.at[1, 2 * m + odd], far, c_recv.at[1, 2 * m + odd])
            for d in range(SIDE):
                for p in range(3):
                    span = pl.ds(cuts[p], cuts[p + 1] - cuts[p])
                    for n, g, i, ds in list(members(m, p, d))[2 * odd:2 * odd + 2]:
                        start = i * cap if isinstance(i, int) else pl.multiple_of(i * cap, cap)
                        pltpu.make_async_copy(back.at[moved(ds[ROUTES[p][1]]), g, pl.ds(start, cap), span],
                                              land.at[pl.ds((4 * d + n) * cap, cap), span], m_sem).start()
        pltpu.make_async_copy(land, land, m_sem).wait()
        for d in (2, 1, 3, 0):
            for p in (2, 0, 1):
                lo, hi = cuts[p], cuts[p + 1]
                a = ROUTES[p][2]
                _, b, c = OUT_ROUTES[a]
                tall = []
                for n, g, i, ds in members(m, p, d):
                    row = pl.ds(back_of(ds[b]) * 4 + back_of(ds[c]), 1)
                    here = keys[a, (SIDE - d) % SIDE, row, :] == slot
                    left = gates[a, (SIDE - d) % SIDE, row, :]
                    wide = []
                    for _ in range(3):
                        piece = left.astype(BF16).astype(F32)
                        left = left - piece
                        wide.append(jnp.where(here, piece, 0.0))
                    tall.append(jnp.concatenate(wide, axis=1))
                weight = jnp.concatenate(tall, axis=0).astype(BF16)
                parts = lax.dot_general(weight, land[4 * d * cap:4 * (d + 1) * cap, lo:hi], (((0,), (0,)), ((), ())),
                                        preferred_element_type=F32)
                acc[d, :, lo:hi] += parts[:tok] + parts[tok:2 * tok] + parts[2 * tok:]
                if d:
                    @pl.when(m == GROUPS // 2 - 1)
                    def _():
                        for part in ((0, 1) if d == 2 else (1,) if d == 1 else (0,)):
                            partial_copy(p, d, part).start()

    def mix_odd(g):
        pl.when(lax.rem(g, 2) == 1)(lambda: mix(lax.div(g, 2)))

    own[3].wait()
    own[4].wait()
    for a in range(3):
        plane_keys(a, 0)
        own[a].wait()
        acc[0, :, cuts[a]:cuts[a + 1]] = gathered[a][0].astype(F32)
    early_picks(0)
    acc[1:] = jnp.zeros((SIDE - 1, tok, dim), F32)
    for k in (1, 3):
        for a in range(3):
            for c in ag_copies(a, k):
                c.wait_recv()
            pass_on(a, k).start()
    for k in (1, 3, 2):
        for a in range(3):
            if k == 2:
                for c in ag_copies(a, k):
                    c.wait_recv()
                pass_on(a, 1).wait_recv()
                pass_on(a, 3).wait_recv()
            plane_keys(a, k)
        early_picks(k)
    for a in range(3):
        for k in (2, 1, 3):
            for c in ag_copies(a, k):
                c.wait_send()
        pass_on(a, 1).wait_send()
        pass_on(a, 3).wait_send()

    def in_turn(r, lag, step):
        g = r - lag
        pl.when((g >= 0) & (g < GROUPS))(lambda: step(g))

    @pl.loop(0, GROUPS + 3)
    def _(r):
        @pl.when(r == 1)
        def _():
            for c in w_copies:
                c.wait()

        in_turn(r, 0, forward)
        in_turn(r, 1, fetch)
        pl.when(r + LEAD < GROUPS)(lambda: pick(r + LEAD))
        in_turn(r, 1, experts)
        in_turn(r, 2, second_hops)
        in_turn(r, 3, mix_odd)

    for p in (2, 0, 1):
        join(p)
    for p in (0, 1, 2):
        lo, hi = cuts[p], cuts[p + 1]
        for part in range(2):
            partial_copy(p, 2, part).wait_send()
            for d in (1, 3):
                partial_copy(p, d, part).wait()
        out_ref[:, lo:hi] = (acc[0, :, lo:hi] + partial[0, :, lo:hi] + partial[2, :, lo:hi]).astype(BF16)
    for ring in range(RING):
        wait_rows(stage.at[ring], far, d_send.at[ring])
        wait_rows(outs.at[ring], far, c_send.at[ring])
    for sem in (d_relay, c_relay):
        part = back.at[0, :, pl.ds(0, far)]
        pltpu.make_async_copy(part, part, sem).wait()


def solution(mesh):
    row_spec = P(('rep', 'ep', 'fsdp'), None)

    def device_step(tokens, expert_idx, gates, w_gate, w_up, w_down):
        tok, top_k = expert_idx.shape
        dim = tokens.shape[1]
        half, width = w_gate.shape[1:]
        cap = (2 * tok * top_k + N_EXP - 1) // N_EXP
        cuts = (0, 640, 1280, dim)
        rows = PER * cap
        idx_t = expert_idx.T
        gate_t = gates.T
        vmem = pl.BlockSpec(memory_space=pltpu.VMEM)
        hbm = pl.BlockSpec(memory_space=pl.ANY)
        sem = pltpu.SemaphoreType.DMA
        out, _, _ = pl.pallas_call(
            functools.partial(layer_kernel, cap, cuts),
            out_shape=(jax.ShapeDtypeStruct((tok, dim), BF16), jax.ShapeDtypeStruct((2, GROUPS, rows, dim), BF16),
                       jax.ShapeDtypeStruct((2, GROUPS, rows, dim), BF16)),
            in_specs=[hbm] * 6,
            out_specs=(vmem, hbm, hbm),
            scratch_shapes=[pltpu.VMEM((dim, 2 * width), BF16), pltpu.VMEM((width, dim), BF16)]
            + [pltpu.VMEM((SIDE, tok, cuts[a + 1] - cuts[a]), BF16) for a in range(3)]
            + [pltpu.VMEM((3, 3, top_k, tok), jnp.int32), pltpu.VMEM((3, 3, top_k, tok), F32), pltpu.VMEM((top_k, tok), jnp.int32), pltpu.VMEM((top_k, tok), F32), pltpu.VMEM((3, SIDE, 16, tok), F32), pltpu.VMEM((3, SIDE, 16, tok), F32),
               pltpu.VMEM((SIDE, tok, dim), F32), pltpu.VMEM((SIDE - 1, tok, dim), F32), pltpu.VMEM((RING, rows, dim), BF16),
               pltpu.VMEM((rows, dim), BF16), pltpu.VMEM((RING, rows, dim), BF16), pltpu.VMEM((2 * rows, dim), BF16),
               sem((3, 3)), sem((3, 3)), sem((3, 3)), sem((3, 3)), sem((3, 3)), sem((3, 3)), sem((3, 2)), sem((3, 2)), sem((5,)),
               sem((3,)), sem((3,)), sem((3,)),
               sem((RING,)), sem((GROUPS,)), sem((2, GROUPS)), sem,
               sem((RING,)), sem((GROUPS,)), sem((2, GROUPS)), sem, sem((3, 2)), sem((3, 2)), sem((3, 2, 2)), sem((3, 2, 2)), sem, sem],
            compiler_params=pltpu.CompilerParams(collective_id=0, has_side_effects=True, vmem_limit_bytes=63 * 1024 * 1024),
            name="moe_layer",
        )(idx_t, gate_t, tokens, w_gate[0], w_up[0], w_down[0])
        return out

    return jax.shard_map(device_step, mesh=mesh, in_specs=(row_spec, row_spec, row_spec, P('ep', 'fsdp', None), P('ep', 'fsdp', None), P('ep', None, 'fsdp')), out_specs=row_spec, check_vma=False)
```
